32 devices in a mesh: grp: 2 (over x), tm: 16 (over z, y, core).
Axes of the slice: x: 2, y: 2, z: 4, core: 2. Of those that a mesh axis runs over, the one named last changes fastest.
Arguments:
- visibilities: float32 [2048, 2, 16, 1024], P('tm', None, 'grp'), parts along dimension 2, may hold values from -6 to 6
- redundancy: int32 [2048], P('grp'), parts along dimension 0, may hold values from 0 to 511, as said below
- mode_counts: int32 [2048], P('tm'), may hold values from 4 to 16
- filters: bfloat16 [2048, 2, 16, 16, 512], P('tm', None, None, 'grp'), parts along dimension 3, may hold values from -0.0625 to 0.0625
Outputs:
- mmodes: float32 [2048, 2, 16, 512], P('tm', None, 'grp'), parts along dimension 2
- modes: float32 [2048, 2, 32], P('tm', None, 'grp'), parts along dimension 2
The draws below stay inside these ranges and needn't reach their ends.
There are 2 independent parts, one for each index of `grp`. The reference program is written for one: setup_inputs(seed, part) draws one part's arguments, and reference() takes and returns one part's arrays. A program takes and returns all parts, laid end to end along the dimension named above; an argument that names none is the same for every part. Nothing has to cross between parts.
Inputs may be any that keep to these rules, and one draw needn't show every extreme that they name: `redundancy`: each of the 512 unique baselines is named by at least one raw baseline.
All inputs are finite; a program needn't handle non-finite values.
Results may differ from the reference program's by a relative error of at most 0.0029.
Values sent between devices are 32-bit elements; how exact they have to be, the bound alone decides.
A program may use at most 128 MiB of HBM per device.

```python
import jax
import jax.numpy as jnp
from jax import lax

TIMES = 2048
NRAW = 1024
B = 512
F = 8
K = 16


def draw_redundancy(key, part):
    base_key = jax.random.fold_in(key, 11)
    perm_key, extra_key, order_key = jax.random.split(base_key, 3)
    covering = jax.random.permutation(perm_key, B).astype(jnp.int32)
    extras = jax.random.randint(extra_key, (NRAW - B,), 0, B).astype(jnp.int32)
    combined = jnp.concatenate([covering, extras])
    shuffle = jax.random.permutation(order_key, NRAW)
    return combined[shuffle].astype(jnp.int32)


def place_ends(result, key, smallest, top_value):
    place = [jax.random.randint(jax.random.fold_in(key, axis), (), 0, length) for axis, length in enumerate(result.shape)]
    main_axis = result.shape.index(max(result.shape))
    next_to = place[:main_axis] + [(place[main_axis] + 1) % result.shape[main_axis]] + place[main_axis + 1:]
    return result.at[tuple(place)].set(smallest).at[tuple(next_to)].set(top_value)


def level_of(key, dims, shards, low, top_value):
    level = 1.0
    for position, parts in shards:
        steps = jax.random.uniform(jax.random.fold_in(jax.random.fold_in(key, 6), position), (parts,), jnp.float32, low / len(shards), top_value / len(shards))
        level = level * jnp.repeat(jnp.exp(steps), dims[position] // parts).reshape((-1,) + (1,) * (len(dims) - 1 - position))
    return level


def scatter_about(key, dims, width, bound, cuts=(), kind=jnp.bfloat16):
    factor_of = level_of(key, dims, cuts, -0.22, 0.18) if cuts else 1.0
    entries = jax.random.normal(key, dims, jnp.float32) * width * factor_of
    return jnp.minimum(jnp.maximum(entries, -bound), bound).astype(kind)


def setup_inputs(seed: int = 0, part: int = 0) -> dict:
    streams_of = jax.random.split(jax.random.key(seed), 5)
    part_splits = jax.random.split(jax.random.fold_in(streams_of[4], part), 5)
    return {
        "visibilities": scatter_about(part_splits[0], (TIMES, 2, F, NRAW), 1.0, 6.0, ((0, 16),), jnp.float32),
        "redundancy": draw_redundancy(jax.random.fold_in(jax.random.fold_in(streams_of[4], part), 71), part),
        "mode_counts": place_ends(jax.random.randint(streams_of[2], (TIMES,), K // 4, K + 1), jax.random.fold_in(streams_of[2], 1), K // 4, K).astype(jnp.int32),
        "filters": scatter_about(part_splits[3], (TIMES, 2, K, F, B), (2 * F * B) ** -0.5, 0.0625, ((0, 16),)),
    }


def project(pieces):
    filt_block, data_block = pieces
    products = jnp.einsum("mpkc,mqc->mpqk", filt_block.astype(jnp.float32), data_block, precision=lax.Precision.HIGHEST)
    real_out = products[:, 0, 0] - products[:, 1, 1]
    imag_out = products[:, 0, 1] + products[:, 1, 0]
    return jnp.stack([real_out, imag_out], axis=1)


def reference(visibilities, redundancy, mode_counts, filters):
    uniques = filters.shape[4]
    kept = filters.shape[2]
    members = (redundancy[:, None] == jnp.arange(uniques, dtype=jnp.int32)[None, :]).astype(jnp.float32)
    summed = jnp.einsum("tpfr,rb->tpfb", visibilities, members, precision=lax.Precision.HIGHEST)
    averaged = summed / jnp.sum(members, axis=0)
    spectra = jnp.fft.fft(averaged[:, 0] + 1j * averaged[:, 1], axis=0, norm="ortho")
    mmodes = jnp.stack([jnp.real(spectra), jnp.imag(spectra)], axis=1).astype(jnp.float32)
    rounded = lax.optimization_barrier(mmodes.astype(jnp.bfloat16)).astype(jnp.float32)
    blocks = TIMES // 64
    data_blocks = rounded.reshape(blocks, 64, 2, -1)
    filt_blocks = filters.reshape(blocks, 64, 2, kept, -1)
    coefs = lax.map(project, (filt_blocks, data_blocks)).reshape(TIMES, 2, kept)
    kept_mask = jnp.arange(kept, dtype=jnp.int32)[None, :] < mode_counts[:, None]
    modes = jnp.where(kept_mask[:, None, :], coefs, 0.0).astype(jnp.float32)
    return mmodes, modes
```

```python
import functools

import numpy as np
import jax
import jax.numpy as jnp
from jax import lax
from jax.experimental import pallas as pl
from jax.experimental.pallas import tpu as pltpu
from jax.sharding import PartitionSpec as P

MESH = pl.DeviceIdType.MESH
LANES = 128
BLOCKS = 4
RADIX = 4
NT = (((1,), (1,)), ((), ()))


def split_bf16(x):
    high = x.astype(jnp.bfloat16)
    return high, (x - high.astype(jnp.float32)).astype(jnp.bfloat16)


def rounded(x):
    return x.astype(jnp.bfloat16).astype(jnp.float32)[None]


def slab_factors(span, length):
    i = np.arange(span)
    side = np.sin(np.pi * (i[:-1] + 1) / length) * np.sin(np.pi * (span - 1 - i[:-1]) / length)
    middle = -np.cos(np.pi * (2 * i + 1 - span) / length) * np.cos(np.pi * span / length)
    _, basis = np.linalg.eigh(np.diag(middle) + np.diag(side, 1) + np.diag(side, -1))
    basis = basis[:, ::-1]
    mid = (span - 1) / 2
    at = i - mid
    basis = basis * np.where((1 + at / span) @ basis < 0, -1.0, 1.0)
    image = np.exp(-2j * np.pi / length * np.outer(at, at)) @ basis
    sizes = np.sqrt(np.sum(np.abs(image) ** 2, axis=0))
    rank = int(np.sum(sizes > sizes[0] * 2.0 ** -24))
    rank = -(-rank // 4) * 4
    dec = image[:, :rank] * np.exp(-2j * np.pi * mid / length * i)[:, None]
    enc = basis[:, :rank].T * np.exp(-2j * np.pi * mid / length * at)
    return dec, enc


def split_rows(rank):
    main = rank // 8 * 8
    return main, 2 * rank


def real_rows(re, im):
    main, _ = split_rows(re.shape[0])
    return np.concatenate([re[:main], im[:main], re[main:], im[main:]], axis=0)


def stacked_tables(slab, local):
    span = slab * local
    length = RADIX * span
    dec, enc = slab_factors(span, length)
    rank = enc.shape[0]
    rows = -(-2 * rank // 16) * 16
    deep = -(-2 * rank // LANES) * LANES
    per = local // RADIX
    bf16 = jnp.bfloat16

    def halves(a):
        high = a.astype(np.float32).astype(bf16)
        low = (a.astype(np.float32) - high.astype(np.float32)).astype(bf16)
        return np.concatenate([high, low], axis=0)

    enc_tables, dec_tables = [], []
    for r in range(RADIX):
        t = np.arange(span).reshape(slab, per, RADIX)[:, :, r]
        part = enc[:, t]
        cols = np.stack(
            [real_rows(part.real, part.imag), real_rows(-part.imag, part.real)], axis=2
        ).reshape(2 * rank, slab * 2 * per)
        enc_tables.append(halves(np.pad(cols, ((0, rows - 2 * rank), (0, 0)))))
        part = dec[t] * length ** -0.5
        part = np.moveaxis(part, -1, 0)
        cols = np.stack(
            [real_rows(part.real, -part.imag), real_rows(part.imag, part.real)], axis=2
        ).reshape(2 * rank, slab * 2 * per)
        dec_tables.append(halves(np.pad(cols, ((0, deep - 2 * rank), (0, 0))).T))
    return rank, jnp.asarray(np.stack(enc_tables)), jnp.asarray(np.stack(dec_tables))


def dft_radix(load, store, rank):
    main, total = split_rows(rank)

    def spread(g, turn):
        s02, d02 = g[0] + g[2], g[0] - g[2]
        s13, d13 = g[1] + g[3], turn(g[1] - g[3])
        return s02 + s13, d02 + d13, s02 - s13, d02 - d13

    def pair(q, carry):
        re = pl.ds(pl.multiple_of(q * 8, 8), 8)
        im = pl.ds(pl.multiple_of(main + q * 8, 8), 8)
        a = [load(k, re) for k in range(4)]
        b = [load(k, im) for k in range(4)]
        sa, da, sb, db = a[0] + a[2], a[0] - a[2], b[0] + b[2], b[0] - b[2]
        ta, ea, tb, eb = a[1] + a[3], a[1] - a[3], b[1] + b[3], b[1] - b[3]
        for k, (x, y) in enumerate(
            ((sa + ta, sb + tb), (da + eb, db - ea), (sa - ta, sb - tb), (da - eb, db + ea))
        ):
            store(k, re, x)
            store(k, im, y)
        return carry

    lax.fori_loop(0, main // 8, pair, 0, unroll=3)
    if total > 2 * main:
        at = pl.ds(2 * main, 8)
        sign = jnp.where(lax.broadcasted_iota(jnp.int32, (8, LANES), 0) < 4, 1.0, -1.0)
        out = spread([load(k, at) for k in range(4)], lambda v: pltpu.roll(v, 4, 0) * sign)
        for k in range(4):
            store(k, at, out[k])


def stacked_dot(table, x):
    high, low = split_bf16(x)
    out = jnp.dot(table, jnp.concatenate([high, low], axis=1), preferred_element_type=jnp.float32)
    out = out[:, :LANES] + out[:, LANES:]
    half = out.shape[0] // 2
    return out[:half] + out[half:]


def fused_kernel(
    n, local, chans, uniq, kept, rank,
    vis_ref, filt_ref, enc_hbm, dec_hbm, red_ref, mm_ref, modes_ref,
    vis_buf, wt, avg, send, recv_a, mix, send_b, recv_b, back, recv_c, lay, part, filt, enc, dec,
    load_sem, tab_sem, a0s, a0r, as_, ar, bs, br, cs, cr, filt_sem, out_sem,
):
    slab = n // RADIX
    me = lax.axis_index("tm")
    z, c = lax.div(me, slab), lax.rem(me, slab)
    tiles = uniq // LANES
    per_dev = chans // slab
    steps = tiles * per_dev
    tb = local // BLOCKS
    vb = tb // RADIX
    per = local // RADIX
    width = 2 * chans
    total = 2 * rank

    def load(i, r):
        return pltpu.make_async_copy(
            vis_ref.at[pl.ds(i * vb, vb), r], vis_buf.at[i, r], load_sem.at[i, r]
        )

    def fetch(j, slot):
        return pltpu.make_async_copy(
            filt_ref.at[:, :, :, :, pl.ds(pl.multiple_of(j * LANES, LANES), LANES)],
            filt.at[slot],
            filt_sem.at[slot],
        )

    table_copies = [
        pltpu.make_async_copy(enc_hbm, enc, tab_sem.at[0]),
        pltpu.make_async_copy(dec_hbm, dec, tab_sem.at[1]),
    ]
    for i in range(BLOCKS):
        for r in range(RADIX):
            load(i, r).start()
    for copy in table_copies:
        copy.start()

    def in_slab(o):
        return z * slab + lax.rem(c + o, slab)

    def across(o):
        return lax.rem(z + o, RADIX) * slab + c

    barrier = pltpu.get_barrier_semaphore()
    peers = [in_slab(o) for o in range(1, slab)] + [across(o) for o in range(1, RADIX)]
    for peer in peers:
        pl.semaphore_signal(barrier, inc=1, device_id={"tm": peer}, device_id_type=MESH)

    wt[...] = (
        lax.broadcasted_iota(jnp.int32, wt.shape, 0) == red_ref[...]
    ).astype(jnp.float32).astype(jnp.bfloat16)
    ones = jnp.ones((8, wt.shape[1]), jnp.bfloat16)
    counts = lax.dot_general(ones, wt[...], NT, preferred_element_type=jnp.float32)
    inverse = 1.0 / counts[0:1]

    def remote(src, dst, ssem, rsem, peer):
        return pltpu.make_async_remote_copy(
            src_ref=src, dst_ref=dst, send_sem=ssem, recv_sem=rsem,
            device_id={"tm": peer}, device_id_type=MESH,
        )

    def first_part(i, o):
        at = pl.ds(i * vb, vb)
        dest = lax.rem(c + o, slab)
        return remote(
            send.at[0, dest, :, :, at, :], recv_a.at[0, c, :, :, at, :],
            a0s.at[i, o], a0r.at[i, o], in_slab(o),
        )

    def first(s, o):
        dest = lax.rem(c + o, slab)
        return remote(send.at[s, dest], recv_a.at[s, c], as_.at[s, o], ar.at[s, o], in_slab(o))

    def second(s, o):
        dest = lax.rem(z + o, RADIX)
        return remote(send_b.at[s, dest], recv_b.at[s, z], bs.at[s, o], br.at[s, o], across(o))

    def third(s, o):
        dest = lax.rem(c + o, slab)
        return remote(send.at[s, dest], recv_c.at[s, c], cs.at[s, o], cr.at[s, o], in_slab(o))

    for i in range(BLOCKS):
        for r in range(RADIX):
            load(i, r).wait()
        high, low = split_bf16(vis_buf[i].reshape(tb * width, vis_buf.shape[-1]))
        summed = lax.dot_general(high, wt[...], NT, preferred_element_type=jnp.float32)
        summed += lax.dot_general(low, wt[...], NT, preferred_element_type=jnp.float32)
        mean = summed * inverse
        for j in range(tiles):
            avg[j] = mean[:, j * LANES:(j + 1) * LANES]
        for j in range(tiles):
            for f in range(chans):
                for r in range(RADIX):
                    for p in range(2):
                        send[j * per_dev + f % per_dev, f // per_dev, r, p, i * vb:(i + 1) * vb, :] = avg[
                            j, pl.ds(r * vb * width + p * chans + f, vb, stride=width), :
                        ]
        if i == 0:
            pl.semaphore_wait(barrier, len(peers))
        for o in range(1, slab):
            first_part(i, o).start()
    for s in range(1, steps):
        for o in range(1, slab):
            first(s, o).start()
    for j in range(2):
        fetch(j, j).start()

    def keep(s, carry):
        recv_a[s, c] = send[s, c]
        return carry

    lax.fori_loop(0, steps, keep, 0)
    part[...] = jnp.zeros_like(part)
    for copy in table_copies:
        copy.wait()

    def encode(s):
        for r in range(RADIX):
            x = recv_a[s, :, r].reshape(slab * 2 * per, LANES)
            mix[r] = stacked_dot(enc[r], x)[:mix.shape[1]]

        def put(k, at, v):
            send_b[s, k, at, :] = v

        dft_radix(lambda k, at: mix[k, at, :], put, rank)
        recv_b[s, z] = send_b[s, z]
        for o in range(1, RADIX):
            second(s, o).start()

    def decode(s):
        for o in range(1, RADIX):
            second(s, o).wait_recv()

        def put(k, at, v):
            back[k, at, :] = v

        dft_radix(lambda k, at: recv_b[s, k, at, :], put, rank)
        for r in range(RADIX):
            y = stacked_dot(dec[r], back[r]).reshape(slab, 2, per, LANES)
            for d in range(slab):
                send[s, d, r] = y[d]
        recv_c[s, c] = send[s, c]
        for o in range(1, slab):
            third(s, o).start()

    def place(s, j, f2):
        for o in range(1, slab):
            third(s, o).wait_recv()

        def one(d, carry):
            for r in range(RADIX):
                for p in range(2):
                    start = (r * 2 + p) * chans + f2 + d * per_dev
                    lay[j, pl.ds(start, per, stride=RADIX * width), :] = recv_c[s, d, r, p]
            return carry

        lax.fori_loop(0, slab, one, 0)

    def write(j):
        return pltpu.make_async_copy(
            lay.at[j], mm_ref.at[:, pl.ds(pl.multiple_of(j * LANES, LANES), LANES)], out_sem.at[j]
        )

    def project(j, slot, m):
        at = pl.multiple_of(m * width, width)
        x0 = rounded(lay[j, pl.ds(at, chans), :])
        x1 = rounded(lay[j, pl.ds(at + chans, chans), :])
        f0 = filt[slot, m, 0].astype(jnp.float32)
        f1 = filt[slot, m, 1].astype(jnp.float32)
        part[m, 0] += jnp.sum(f0 * x0 - f1 * x1, axis=1)
        part[m, 1] += jnp.sum(f0 * x1 + f1 * x0, axis=1)

    def finish(j):
        for f2 in range(per_dev):
            place(j * per_dev + f2, j, f2)
        write(j).start()
        slot = lax.rem(j, 2)
        fetch(j, slot).wait()

        def one(m, carry):
            project(j, slot, m)
            return carry

        lax.fori_loop(0, local, one, 0)

        @pl.when(j + 2 < tiles)
        def _():
            fetch(j + 2, slot).start()

    back[:, total:, :] = jnp.zeros((RADIX, back.shape[1] - total, LANES), jnp.float32)
    for i in range(BLOCKS):
        for o in range(1, slab):
            first_part(i, o).wait_recv()
    encode(0)
    for i in range(BLOCKS):
        for o in range(1, slab):
            first_part(i, o).wait_send()

    def step(d, carry):
        for q in (1, 2):
            e = 2 * d + q

            @pl.when(e < steps)
            def _():
                for o in range(1, slab):
                    first(e, o).wait_recv()
                encode(e)

        @pl.when((d >= per_dev + 1) & (lax.rem(d, per_dev) == per_dev - 1))
        def _():
            finish(lax.div(d - per_dev - 1, per_dev))

        @pl.when(d > 0)
        def _():
            for o in range(1, slab):
                first(d, o).wait_send()

        decode(d)
        return carry

    lax.fori_loop(0, steps, step, 0)

    j = tiles - 1
    for f2 in range(per_dev):
        place(j * per_dev + f2, j, f2)
    write(j).start()
    fetch(j, j % 2).wait()
    group = modes_ref.shape[2] // (2 * kept)

    def last(k, carry):
        def one(m, inner):
            project(j, j % 2, k * group + m)
            return inner

        lax.fori_loop(0, group, one, 0)
        sums = part[pl.ds(k * group, group)].reshape(group * 2 * kept, LANES)
        high, low = split_bf16(sums)
        whole = lax.dot_general(
            jnp.ones((8, 2 * LANES), jnp.bfloat16), jnp.concatenate([high, low], axis=1), NT,
            preferred_element_type=jnp.float32,
        )
        modes_ref[k] = whole[0:1]
        return carry

    lax.fori_loop(0, modes_ref.shape[0], last, 0)

    def drain(s, carry):
        for o in range(1, RADIX):
            second(s, o).wait_send()
        for o in range(1, slab):
            third(s, o).wait_send()
        return carry

    lax.fori_loop(0, steps, drain, 0)
    for t in range(tiles):
        write(t).wait()


def fits(n, local, chans, raw, uniq, kept):
    slab = n // RADIX
    return (
        n == RADIX * slab
        and slab > 1
        and chans == 8
        and chans % slab == 0
        and local % (BLOCKS * RADIX * 8) == 0
        and slab * local * 2 // RADIX <= 2 * LANES
        and raw % LANES == 0
        and raw <= 8 * LANES
        and uniq % LANES == 0
        and 2 * LANES <= uniq <= 4 * LANES
        and kept == 16
        and chans // slab == 2
    )


def fused_device(visibilities, redundancy, mode_counts, filters):
    n = lax.axis_size("tm")
    local, _, chans, raw = visibilities.shape
    uniq, kept = filters.shape[4], filters.shape[2]
    slab = n // RADIX
    tiles = uniq // LANES
    per_dev = chans // slab
    steps = tiles * per_dev
    per = local // RADIX
    width = 2 * chans
    tb = local // BLOCKS
    rank, enc, dec = stacked_tables(slab, local)
    total = 2 * rank
    vmem = pl.BlockSpec(memory_space=pltpu.VMEM)
    hbm = pl.BlockSpec(memory_space=pl.ANY)
    f32, bf16 = jnp.float32, jnp.bfloat16
    dma = pltpu.SemaphoreType.DMA
    group = 16
    mmodes, flat = pl.pallas_call(
        functools.partial(fused_kernel, n, local, chans, uniq, kept, rank),
        out_shape=(
            jax.ShapeDtypeStruct((local * width, uniq), f32),
            jax.ShapeDtypeStruct((local // group, 1, group * 2 * kept), f32),
        ),
        in_specs=[hbm] * 4 + [vmem],
        out_specs=(hbm, vmem),
        scratch_shapes=[
            pltpu.VMEM((BLOCKS, RADIX, tb // RADIX, width, raw), f32),
            pltpu.VMEM((uniq, raw), bf16),
            pltpu.VMEM((tiles, tb * width, LANES), f32),
            pltpu.VMEM((steps, slab, RADIX, 2, per, LANES), f32),
            pltpu.VMEM((steps, slab, RADIX, 2, per, LANES), f32),
            pltpu.VMEM((RADIX, total, LANES), f32),
            pltpu.VMEM((steps, RADIX, total, LANES), f32),
            pltpu.VMEM((steps, RADIX, total, LANES), f32),
            pltpu.VMEM((RADIX, dec.shape[2], LANES), f32),
            pltpu.VMEM((steps, slab, RADIX, 2, per, LANES), f32),
            pltpu.VMEM((tiles, local * width, LANES), f32),
            pltpu.VMEM((local, 2, kept, LANES), f32),
            pltpu.VMEM((2, local, 2, kept, chans, LANES), bf16),
            pltpu.VMEM(enc.shape, bf16),
            pltpu.VMEM(dec.shape, bf16),
            dma((BLOCKS, RADIX)),
            dma((2,)),
            dma((BLOCKS, slab)),
            dma((BLOCKS, slab)),
            dma((steps, slab)),
            dma((steps, slab)),
            dma((steps, RADIX)),
            dma((steps, RADIX)),
            dma((steps, slab)),
            dma((steps, slab)),
            dma((2,)),
            dma((tiles,)),
        ],
        compiler_params=pltpu.CompilerParams(
            collective_id=0, has_side_effects=True, vmem_limit_bytes=67043328 - 2**17
        ),
        name="fused",
    )(
        visibilities.reshape(local // RADIX, RADIX, width, raw),
        filters, enc, dec, redundancy.reshape(1, raw),
    )
    coefs = flat.reshape(local, 2, kept)
    kept_mask = lax.broadcasted_iota(jnp.int32, (local, kept), 1) < mode_counts[:, None]
    return mmodes.reshape(local, 2, chans, uniq), jnp.where(kept_mask[:, None, :], coefs, 0.0)


def phase_table(numer, period):
    phases = 2.0 * jnp.pi / period * numer.astype(jnp.float32)
    return (jnp.cos(phases), jnp.sin(phases))


def apply_stacked(cosine, sine_table, stacked, width):
    cos_part = jnp.dot(
        cosine, stacked, precision=lax.Precision.HIGHEST, preferred_element_type=jnp.float32
    )
    sin_part = jnp.dot(
        sine_table, stacked, precision=lax.Precision.HIGHEST, preferred_element_type=jnp.float32
    )
    real_out = cos_part[:, :width] + sin_part[:, width:]
    imag_out = cos_part[:, width:] - sin_part[:, :width]
    return jnp.concatenate([real_out, imag_out], axis=1)


def factored_transform(stacked, width):
    length = stacked.shape[0]
    radix_size = 64
    inner_size = length // radix_size
    outer_row = lax.broadcasted_iota(jnp.int32, (radix_size, radix_size), 0)
    outer_col = lax.broadcasted_iota(jnp.int32, (radix_size, radix_size), 1)
    cosine, sine_table = phase_table(outer_row * outer_col % radix_size, radix_size)
    grouped = stacked.reshape(radix_size, inner_size, 2, width)
    grouped = jnp.transpose(grouped, (0, 2, 1, 3)).reshape(radix_size, 2 * inner_size * width)
    section = apply_stacked(cosine, sine_table, grouped, inner_size * width)
    section = section.reshape(radix_size, 2, inner_size, width)
    section_real = section[:, 0]
    section_imag = section[:, 1]
    twist_row = lax.broadcasted_iota(jnp.int32, (radix_size, inner_size, 1), 0)
    twist_col = lax.broadcasted_iota(jnp.int32, (radix_size, inner_size, 1), 1)
    twist_cos, twist_sin = phase_table(twist_row * twist_col, length)
    turned_real = section_real * twist_cos + section_imag * twist_sin
    turned_imag = section_imag * twist_cos - section_real * twist_sin
    turned = jnp.stack([turned_real, turned_imag], axis=0)
    turned = jnp.transpose(turned, (2, 0, 1, 3)).reshape(inner_size, 2 * radix_size * width)
    inner_row = lax.broadcasted_iota(jnp.int32, (inner_size, inner_size), 0)
    inner_col = lax.broadcasted_iota(jnp.int32, (inner_size, inner_size), 1)
    cosine2, sine_table2 = phase_table(inner_row * inner_col % inner_size, inner_size)
    final = apply_stacked(cosine2, sine_table2, turned, radix_size * width)
    final = final.reshape(inner_size, 2, radix_size, width)
    return jnp.transpose(final, (0, 2, 1, 3)).reshape(length, 2 * width)


def transform(columns):
    length, _, width = columns.shape
    stacked = columns.reshape(length, 2 * width)
    result = factored_transform(stacked, width)
    scale = 1.0 / jnp.sqrt(jnp.float32(length))
    return (result * scale).reshape(length, 2, width)


def on_device(visibilities, redundancy, mode_counts, filters):
    groups = lax.axis_size("tm")
    local_times, _, channels, raw_count = visibilities.shape
    uniques = filters.shape[4]
    kept = filters.shape[2]
    if fits(groups, local_times, channels, raw_count, uniques, kept):
        return fused_device(visibilities, redundancy, mode_counts, filters)
    unique_block = uniques // groups
    members = (
        redundancy[:, None] == lax.broadcasted_iota(jnp.int32, (raw_count, uniques), 1)
    ).astype(jnp.float32)
    weights = members / jnp.sum(members, axis=0, keepdims=True)
    flat_rows = visibilities.reshape(local_times, 2 * channels, raw_count)
    blocked_weights = weights.reshape(raw_count, groups, unique_block)
    packed = jnp.einsum(
        "tqr,rjc->tjqc",
        flat_rows,
        blocked_weights,
        precision=lax.Precision.HIGHEST,
        preferred_element_type=jnp.float32,
    )
    packed = packed.reshape(local_times, groups, 2 * channels * unique_block)
    arrived = lax.all_to_all(packed, "tm", split_axis=1, concat_axis=0, tiled=True)
    length = arrived.shape[0]
    spectra = transform(arrived.reshape(length, 2, channels * unique_block))
    spectra = spectra.reshape(length, 1, 2 * channels * unique_block)
    regrouped = lax.all_to_all(spectra, "tm", split_axis=0, concat_axis=1, tiled=True)
    regrouped = regrouped.reshape(local_times, groups, 2, channels, unique_block)
    mmodes = jnp.transpose(regrouped, (0, 2, 3, 1, 4)).reshape(local_times, 2, channels, uniques)
    local_modes = mmodes.shape[0]
    rounded = mmodes.astype(jnp.bfloat16).reshape(local_modes, 2, channels * uniques)
    flat_filters = filters.reshape(local_modes, 2, kept, channels * uniques)
    products = jnp.einsum(
        "mpkc,mqc->mpqk", flat_filters, rounded, preferred_element_type=jnp.float32
    )
    real_out = products[:, 0, 0] - products[:, 1, 1]
    imag_out = products[:, 0, 1] + products[:, 1, 0]
    kept_mask = lax.broadcasted_iota(jnp.int32, (local_modes, kept), 1) < mode_counts[:, None]
    modes = jnp.where(kept_mask[:, None, :], jnp.stack([real_out, imag_out], axis=1), 0.0)
    return (mmodes, modes)


def solution(mesh):
    return jax.shard_map(
        on_device,
        mesh=mesh,
        in_specs=(P("tm", None, "grp", None), P("grp"), P("tm"), P("tm", None, None, "grp", None)),
        out_specs=(P("tm", None, "grp", None), P("tm", None, "grp")),
        check_vma=False,
    )
```

```python
import functools

import numpy as np
import jax
import jax.numpy as jnp
from jax import lax
from jax.experimental import pallas as pl
from jax.experimental.pallas import tpu as pltpu
from jax.sharding import PartitionSpec as P

MESH = pl.DeviceIdType.MESH
LANES = 128
BLOCKS = 4
RADIX = 4
AHEAD = 3
SLOTS = 3
NT = (((1,), (1,)), ((), ()))


def split_bf16(x):
    high = x.astype(jnp.bfloat16)
    return high, (x - high.astype(jnp.float32)).astype(jnp.bfloat16)


def rounded(x):
    return x.astype(jnp.bfloat16).astype(jnp.float32)[None]


def slab_factors(span, length):
    i = np.arange(span)
    side = np.sin(np.pi * (i[:-1] + 1) / length) * np.sin(np.pi * (span - 1 - i[:-1]) / length)
    middle = -np.cos(np.pi * (2 * i + 1 - span) / length) * np.cos(np.pi * span / length)
    _, basis = np.linalg.eigh(np.diag(middle) + np.diag(side, 1) + np.diag(side, -1))
    basis = basis[:, ::-1]
    mid = (span - 1) / 2
    at = i - mid
    basis = basis * np.where((1 + at / span) @ basis < 0, -1.0, 1.0)
    image = np.exp(-2j * np.pi / length * np.outer(at, at)) @ basis
    sizes = np.sqrt(np.sum(np.abs(image) ** 2, axis=0))
    rank = int(np.sum(sizes > sizes[0] * 2.0 ** -24))
    rank = -(-rank // 4) * 4
    dec = image[:, :rank] * np.exp(-2j * np.pi * mid / length * i)[:, None]
    enc = basis[:, :rank].T * np.exp(-2j * np.pi * mid / length * at)
    return dec, enc


def split_rows(rank):
    main = rank // 8 * 8
    return main, 2 * rank


def real_rows(re, im):
    main, _ = split_rows(re.shape[0])
    return np.concatenate([re[:main], im[:main], re[main:], im[main:]], axis=0)


def stacked_tables(slab, local):
    span = slab * local
    length = RADIX * span
    dec, enc = slab_factors(span, length)
    rank = enc.shape[0]
    rows = -(-2 * rank // 16) * 16
    deep = -(-2 * rank // LANES) * LANES
    per = local // RADIX
    bf16 = jnp.bfloat16

    def halves(a):
        high = a.astype(np.float32).astype(bf16)
        low = (a.astype(np.float32) - high.astype(np.float32)).astype(bf16)
        return np.concatenate([high, low], axis=0)

    enc_tables, dec_tables = [], []
    for r in range(RADIX):
        t = np.arange(span).reshape(slab, per, RADIX)[:, :, r]
        part = enc[:, t]
        cols = np.stack(
            [real_rows(part.real, part.imag), real_rows(-part.imag, part.real)], axis=2
        ).reshape(2 * rank, slab * 2 * per)
        enc_tables.append(halves(np.pad(cols, ((0, rows - 2 * rank), (0, 0)))))
        part = dec[t] * length ** -0.5
        part = np.moveaxis(part, -1, 0)
        cols = np.stack(
            [real_rows(part.real, -part.imag), real_rows(part.imag, part.real)], axis=2
        ).reshape(2 * rank, slab * 2 * per)
        dec_tables.append(halves(np.pad(cols, ((0, deep - 2 * rank), (0, 0))).T))
    return rank, jnp.asarray(np.stack(enc_tables)), jnp.asarray(np.stack(dec_tables))


def dft_radix(load, store, rank):
    main, total = split_rows(rank)

    def spread(g, turn):
        s02, d02 = g[0] + g[2], g[0] - g[2]
        s13, d13 = g[1] + g[3], turn(g[1] - g[3])
        return s02 + s13, d02 + d13, s02 - s13, d02 - d13

    def pair(q, carry):
        re = pl.ds(pl.multiple_of(q * 8, 8), 8)
        im = pl.ds(pl.multiple_of(main + q * 8, 8), 8)
        a = [load(k, re) for k in range(4)]
        b = [load(k, im) for k in range(4)]
        sa, da, sb, db = a[0] + a[2], a[0] - a[2], b[0] + b[2], b[0] - b[2]
        ta, ea, tb, eb = a[1] + a[3], a[1] - a[3], b[1] + b[3], b[1] - b[3]
        for k, (x, y) in enumerate(
            ((sa + ta, sb + tb), (da + eb, db - ea), (sa - ta, sb - tb), (da - eb, db + ea))
        ):
            store(k, re, x)
            store(k, im, y)
        return carry

    lax.fori_loop(0, main // 8, pair, 0, unroll=3)
    if total > 2 * main:
        at = pl.ds(2 * main, 8)
        sign = jnp.where(lax.broadcasted_iota(jnp.int32, (8, LANES), 0) < 4, 1.0, -1.0)
        out = spread([load(k, at) for k in range(4)], lambda v: pltpu.roll(v, 4, 0) * sign)
        for k in range(4):
            store(k, at, out[k])


def stacked_dot(table, x):
    high, low = split_bf16(x)
    out = jnp.dot(table, jnp.concatenate([high, low], axis=1), preferred_element_type=jnp.float32)
    out = out[:, :LANES] + out[:, LANES:]
    half = out.shape[0] // 2
    return out[:half] + out[half:]


def fused_kernel(
    n, local, chans, uniq, kept, rank,
    vis_ref, filt_ref, enc_hbm, dec_hbm, red_ref, counts_ref, mm_ref, modes_ref,
    send, recv_a, mix, send_b, recv_b, back, recv_c, part, turned, enc, dec,
    load_sem, tab_sem, as_, ar, bs, br, cs, cr, filt_sem,
):
    slab = n // RADIX
    me = lax.axis_index("tm")
    z, c = lax.div(me, slab), lax.rem(me, slab)
    tiles = uniq // LANES
    per_dev = chans // slab
    steps = tiles * per_dev
    tb = local // BLOCKS
    vb = tb // RADIX
    per = local // RADIX
    width = 2 * chans
    total = 2 * rank

    table_copies = [
        pltpu.make_async_copy(enc_hbm, enc, tab_sem.at[0]),
        pltpu.make_async_copy(dec_hbm, dec, tab_sem.at[1]),
    ]
    def in_slab(o):
        return z * slab + lax.rem(c + o, slab)

    def across(o):
        return lax.rem(z + o, RADIX) * slab + c

    barrier = pltpu.get_barrier_semaphore()
    peers = [in_slab(o) for o in range(1, slab)] + [across(o) for o in range(1, RADIX)]
    def remote(src, dst, ssem, rsem, peer):
        return pltpu.make_async_remote_copy(
            src_ref=src, dst_ref=dst, send_sem=ssem, recv_sem=rsem,
            device_id={"tm": peer}, device_id_type=MESH,
        )

    def first_part(i, o):
        at = pl.ds(i * vb if isinstance(i, int) else pl.multiple_of(i * vb, vb), vb)
        dest = lax.rem(c + o, slab)
        return remote(
            send.at[0, dest, :, :, at, :], recv_a.at[0, c, :, :, at, :],
            as_.at[0], ar.at[0], in_slab(o),
        )

    def first(s, o):
        dest = lax.rem(c + o, slab)
        return remote(send.at[s, dest], recv_a.at[s, c], as_.at[s], ar.at[s], in_slab(o))

    def second(s, o):
        dest = lax.rem(z + o, RADIX)
        return remote(send_b.at[s, dest], recv_b.at[s, z], bs, br.at[s], across(o))

    def all_first(s):
        some = pl.ds(0, slab - 1)
        return remote(send.at[s, some], recv_a.at[s, some], as_.at[s], ar.at[s], in_slab(1))

    def all_second(s):
        some = pl.ds(0, RADIX - 1)
        return remote(send_b.at[s, some], recv_b.at[s, some], bs, br.at[s], across(1))

    def all_third(s):
        some = pl.ds(0, slab - 1)
        return remote(send.at[s, some], recv_c.at[s, some], cs, cr.at[s], in_slab(1))

    def third(s, o):
        dest = lax.rem(c + o, slab)
        return remote(send.at[s, dest], recv_c.at[s, c], cs, cr.at[s], in_slab(o))

    def encode(s):
        for r in range(RADIX):
            x = recv_a[s, :, r].reshape(slab * 2 * per, LANES)
            mix[r] = stacked_dot(enc[r], x)[:mix.shape[1]]

        def put(k, at, v):
            send_b[s, k, at, :] = v

        dft_radix(lambda k, at: mix[k, at, :], put, rank)
        recv_b[s, z] = send_b[s, z]
        for o in range(1, RADIX):
            second(s, o).start()

    odd = lax.rem(c, 2)
    near, ahead, behind = 1 + 2 * odd, 2 - odd, 3 - odd

    def averages(vis_buf, wt, avg):
        def load(i, r):
            return pltpu.make_async_copy(
                vis_ref.at[pl.ds(i * vb, vb), r], vis_buf.at[i, r], load_sem.at[i]
            )

        for i in range(2):
            for r in range(RADIX):
                load(i, r).start()
        for peer in peers:
            pl.semaphore_signal(barrier, inc=1, device_id={"tm": peer}, device_id_type=MESH)
        wt[...] = (
            lax.broadcasted_iota(jnp.int32, wt.shape, 0) == red_ref[...]
        ).astype(jnp.float32).astype(jnp.bfloat16)
        ones = jnp.ones((8, wt.shape[1]), jnp.bfloat16)
        for i in range(2, BLOCKS):
            for r in range(RADIX):
                load(i, r).start()
        for copy in table_copies:
            copy.start()
        counts = lax.dot_general(ones, wt[...], NT, preferred_element_type=jnp.float32)
        inverse = 1.0 / counts[0:1]

        def average(i, h):
            at = pl.ds(i * vb if isinstance(i, int) else pl.multiple_of(i * vb, vb), vb)
            high, low = split_bf16(vis_buf[i].reshape(tb * width, vis_buf.shape[-1]))
            lanes = slice(h * 2 * LANES, (h + 1) * 2 * LANES)
            members = wt[lanes, :]
            summed = lax.dot_general(high, members, NT, preferred_element_type=jnp.float32)
            summed += lax.dot_general(low, members, NT, preferred_element_type=jnp.float32)
            mean = summed * inverse[:, lanes]
            for q in range(2):
                avg[q] = mean[:, q * LANES:(q + 1) * LANES]
            for q in range(2):
                for f in range(chans):
                    for r in range(RADIX):
                        for p in range(2):
                            s = (h * 2 + q) * per_dev + f % per_dev
                            send[s, f // per_dev, r, p, at, :] = avg[
                                q, pl.ds(r * vb * width + p * chans + f, vb, stride=width), :
                            ]

        def early(i, carry):
            pltpu.make_async_copy(vis_buf.at[i], vis_buf.at[i], load_sem.at[i]).wait()
            average(i, 0)

            @pl.when(i == 0)
            def _():
                pl.semaphore_wait(barrier, len(peers))

            first_part(i, near).start()
            first_part(i, ahead).start()
            return carry

        lax.fori_loop(0, BLOCKS, early, 0)
        for i in range(BLOCKS):
            first_part(i, behind).start()
        recv_a[0, c] = send[0, c]
        for copy in table_copies:
            copy.wait()
        all_first(0).wait_recv()
        for s in (1, 2):
            for o in range(1, slab):
                first(s, o).start()
        encode(0)

        def more(i, carry):
            average(i, 1)
            return carry

        lax.fori_loop(0, BLOCKS, more, 0)

    pl.run_scoped(
        averages,
        pltpu.VMEM((BLOCKS, RADIX, tb // RADIX, width, vis_ref.shape[-1]), jnp.float32),
        pltpu.VMEM((uniq, vis_ref.shape[-1]), jnp.bfloat16),
        pltpu.VMEM((2, tb * width, LANES), jnp.float32),
    )

    pl.run_scoped(
        functools.partial(
            transform_kernel, n, local, chans, uniq, kept, rank, filt_ref, counts_ref, mm_ref, modes_ref,
            send, recv_a, mix, send_b, recv_b, back, recv_c, part, turned, enc, dec,
            first, second, third, all_first, all_second, all_third, encode, filt_sem,
        ),
        pltpu.VMEM((SLOTS, local, 2, kept, chans, LANES), jnp.bfloat16),
    )


def transform_kernel(
    n, local, chans, uniq, kept, rank, filt_ref, counts_ref, mm_ref, modes_ref,
    send, recv_a, mix, send_b, recv_b, back, recv_c, part, turned, enc, dec,
    first, second, third, all_first, all_second, all_third, encode, filt_sem, filt,
):
    slab = n // RADIX
    me = lax.axis_index("tm")
    z, c = lax.div(me, slab), lax.rem(me, slab)
    tiles = uniq // LANES
    per_dev = chans // slab
    steps = tiles * per_dev
    per = local // RADIX
    width = 2 * chans
    total = 2 * rank
    stride = part.shape[0] // local

    def fetch(j):
        at = pl.multiple_of(j * LANES, LANES)
        slot = lax.rem(j, SLOTS)
        return pltpu.make_async_copy(
            filt_ref.at[:, :, :, :, pl.ds(at, LANES)], filt.at[slot], filt_sem.at[slot]
        )

    for j in range(SLOTS):
        fetch(j).start()

    def keep(s, carry):
        recv_a[s, c] = send[s, c]
        return carry

    lax.fori_loop(1, steps, keep, 0)
    part[...] = jnp.zeros_like(part)
    def decode(s):
        all_second(s).wait_recv()

        def put(k, at, v):
            back[k, at, :] = v

        dft_radix(lambda k, at: recv_b[s, k, at, :], put, rank)
        for r in range(RADIX):
            y = stacked_dot(dec[r], back[r]).reshape(slab, 2, per, LANES)
            for d in range(slab):
                send[s, d, r] = y[d]
        recv_c[s, c] = send[s, c]
        for o in range(1, slab):
            third(s, o).start()

    def place(s, j, f2):
        all_third(s).wait_recv()

        def one(d, carry):
            for r in range(RADIX):
                for p in range(2):
                    start = (r * 2 + p) * chans + f2 + d * per_dev
                    mm_ref[j, pl.ds(start, per, stride=RADIX * width), :] = recv_c[s, d, r, p]
            return carry

        lax.fori_loop(0, slab, one, 0)

    def turn(j):
        slot = lax.rem(j, SLOTS)
        fetch(j).wait()

        def one(m, carry):
            for p in range(2):
                turned[p] = filt[slot, m, p].astype(jnp.float32).reshape(kept * chans, LANES)
            for p in range(2):
                for f in range(chans):
                    for g in range(kept // 8):
                        rows = turned[p, pl.ds(g * 8 * chans + f, 8, stride=chans), :]
                        filt[slot, m, p, f * (kept // 8) + g] = rows.astype(jnp.bfloat16)
            return carry

        lax.fori_loop(0, local, one, 0)

    def project(j, f2, m):
        slot = lax.rem(j, SLOTS)
        per_chan = kept // 8
        re = pl.ds(pl.multiple_of(m * stride, 8), kept)
        im = pl.ds(pl.multiple_of(m * stride + kept, 8), kept)
        real, imag = part[re, :], part[im, :]
        for d in range(slab):
            f = d * per_dev + f2
            at = f * per_chan
            x0 = mm_ref[j, pl.ds(m * width + f, 1), :].astype(jnp.bfloat16).astype(jnp.float32)
            x1 = mm_ref[j, pl.ds(m * width + chans + f, 1), :].astype(jnp.bfloat16).astype(jnp.float32)
            f0 = filt[slot, m, 0, pl.ds(at, per_chan)].astype(jnp.float32).reshape(kept, LANES)
            f1 = filt[slot, m, 1, pl.ds(at, per_chan)].astype(jnp.float32).reshape(kept, LANES)
            real += f0 * x0 - f1 * x1
            imag += f0 * x1 + f1 * x0
        part[re, :] = real
        part[im, :] = imag

    def projects(j, f2, low, high):
        def one(m, carry):
            project(j, f2, m)
            return carry

        lax.fori_loop(low, high, one, 0, unroll=2)

    back[:, total:, :] = jnp.zeros((RADIX, back.shape[1] - total, LANES), jnp.float32)

    def later(e):
        all_first(e).wait_recv()

        @pl.when(e + 2 < steps)
        def _():
            for o in range(1, slab):
                first(e + 2, o).start()

        encode(e)

    for e in range(1, AHEAD):
        later(e)

    def step(d, carry):
        @pl.when(d < SLOTS)
        def _():
            turn(d)

        @pl.when(d >= 2)
        def _():
            j, f2 = lax.div(d - 2, per_dev), lax.rem(d - 2, per_dev)
            place(d - 2, j, f2)

            projects(j, f2, 0, local)

            @pl.when((f2 == per_dev - 1) & (j + SLOTS < tiles))
            def _():
                fetch(j + SLOTS).start()

        @pl.when((d >= steps - 2) & (d - (steps - 2) + SLOTS < tiles))
        def _():
            turn(d - (steps - 2) + SLOTS)

        all_first(d).wait_send()
        decode(d)

        @pl.when(d + AHEAD < steps)
        def _():
            later(d + AHEAD)

        return carry

    lax.fori_loop(0, steps, step, 0)

    j = tiles - 1
    lane = lax.broadcasted_iota(jnp.int32, (kept, LANES), 1)

    def gather(q, outs):
        outs = list(outs)
        for i in range(8):
            m = q * 8 + i
            for p in range(2):
                at = pl.ds(pl.multiple_of(m * stride + p * kept, 8), kept)
                row = jnp.sum(part[at, :], axis=1, keepdims=True)
                outs[p] = jnp.where(lane == m, row, outs[p])
        return tuple(outs)

    def last(q, outs):
        outs = gather(jnp.maximum(q - 1, 0), outs)
        for i in range(8):
            project(j, per_dev - 1, q * 8 + i)
        return outs

    for f2 in range(per_dev):
        place(j * per_dev + f2, j, f2)
        if f2 < per_dev - 1:
            projects(j, f2, 0, local)
    zero = jnp.zeros((kept, LANES), jnp.float32)
    outs = lax.fori_loop(0, local // 8, last, (zero, zero))
    outs = gather(local // 8 - 1, outs)
    order = lax.broadcasted_iota(jnp.int32, (kept, LANES), 0)
    for p in range(2):
        modes_ref[p] = jnp.where(order < counts_ref[...], outs[p], 0.0)

    def drain(s, carry):
        all_second(s).wait_send()
        all_third(s).wait_send()
        return carry

    lax.fori_loop(0, steps, drain, 0)


def emit_kernel(mm_ref, modes_ref, out_ref, kept_ref, out_sem):
    tiles, chunks = out_sem.shape
    rows = mm_ref.shape[1] // chunks

    def write(t, q):
        at = pl.ds(q * rows, rows)
        return pltpu.make_async_copy(
            mm_ref.at[t, at], out_ref.at[at, pl.ds(t * LANES, LANES)], out_sem.at[t, q]
        )

    for t in range(tiles):
        for q in range(chunks):
            write(t, q).start()
    kept_ref[...] = modes_ref[...]
    for t in range(tiles):
        for q in range(chunks):
            write(t, q).wait()


def fits(n, local, chans, raw, uniq, kept):
    slab = n // RADIX
    return (
        n == RADIX * slab
        and slab == 4
        and chans == 8
        and chans % slab == 0
        and local % (BLOCKS * RADIX * 8) == 0
        and slab * local * 2 // RADIX <= 2 * LANES
        and raw % LANES == 0
        and raw <= 8 * LANES
        and uniq % LANES == 0
        and uniq == 4 * LANES
        and local == LANES
        and kept == 16
        and chans // slab == 2
    )


def fused_device(visibilities, redundancy, mode_counts, filters):
    n = lax.axis_size("tm")
    local, _, chans, raw = visibilities.shape
    uniq, kept = filters.shape[4], filters.shape[2]
    slab = n // RADIX
    tiles = uniq // LANES
    per_dev = chans // slab
    steps = tiles * per_dev
    per = local // RADIX
    width = 2 * chans
    rank, enc, dec = stacked_tables(slab, local)
    total = 2 * rank
    vmem = pl.BlockSpec(memory_space=pltpu.VMEM)
    hbm = pl.BlockSpec(memory_space=pl.ANY)
    f32, bf16 = jnp.float32, jnp.bfloat16
    dma = pltpu.SemaphoreType.DMA
    stride = 2 * kept
    mm, modes = pl.pallas_call(
        functools.partial(fused_kernel, n, local, chans, uniq, kept, rank),
        out_shape=(
            pltpu.VMEM((tiles, local * width, LANES), f32),
            pltpu.VMEM((2, kept, local), f32),
        ),
        in_specs=[hbm] * 4 + [vmem] * 2,
        out_specs=(pl.BlockSpec(memory_space=pltpu.VMEM), vmem),
        scratch_shapes=[
            pltpu.VMEM((steps, slab, RADIX, 2, per, LANES), f32),
            pltpu.VMEM((steps, slab, RADIX, 2, per, LANES), f32),
            pltpu.VMEM((RADIX, total, LANES), f32),
            pltpu.VMEM((steps, RADIX, total, LANES), f32),
            pltpu.VMEM((steps, RADIX, total, LANES), f32),
            pltpu.VMEM((RADIX, dec.shape[2], LANES), f32),
            pltpu.VMEM((steps, slab, RADIX, 2, per, LANES), f32),
            pltpu.VMEM((local * stride, LANES), f32),
            pltpu.VMEM((2, kept * chans, LANES), f32),
            pltpu.VMEM(enc.shape, bf16),
            pltpu.VMEM(dec.shape, bf16),
            dma((BLOCKS,)),
            dma((2,)),
            dma((steps,)),
            dma((steps,)),
            dma,
            dma((steps,)),
            dma,
            dma((steps,)),
            dma((SLOTS,)),
        ],
        compiler_params=pltpu.CompilerParams(
            collective_id=0, has_side_effects=True, vmem_limit_bytes=59 * 2**20
        ),
        name="fused",
    )(
        visibilities.reshape(local // RADIX, RADIX, width, raw),
        filters, enc, dec, redundancy.reshape(1, raw), mode_counts.reshape(1, local),
    )
    chunks = 8
    mmodes, modes = pl.pallas_call(
        emit_kernel,
        out_shape=(
            jax.ShapeDtypeStruct((local * width, uniq), f32),
            jax.ShapeDtypeStruct((2, kept, local), f32),
        ),
        in_specs=[vmem, vmem],
        out_specs=(hbm, vmem),
        scratch_shapes=[dma((tiles, chunks))],
        compiler_params=pltpu.CompilerParams(vmem_limit_bytes=32 * 2**20),
        name="emit",
    )(mm, modes)
    return mmodes.reshape(local, 2, chans, uniq), jnp.transpose(modes, (2, 0, 1))


def phase_table(numer, period):
    phases = 2.0 * jnp.pi / period * numer.astype(jnp.float32)
    return (jnp.cos(phases), jnp.sin(phases))


def apply_stacked(cosine, sine_table, stacked, width):
    cos_part = jnp.dot(
        cosine, stacked, precision=lax.Precision.HIGHEST, preferred_element_type=jnp.float32
    )
    sin_part = jnp.dot(
        sine_table, stacked, precision=lax.Precision.HIGHEST, preferred_element_type=jnp.float32
    )
    real_out = cos_part[:, :width] + sin_part[:, width:]
    imag_out = cos_part[:, width:] - sin_part[:, :width]
    return jnp.concatenate([real_out, imag_out], axis=1)


def factored_transform(stacked, width):
    length = stacked.shape[0]
    radix_size = 64
    inner_size = length // radix_size
    outer_row = lax.broadcasted_iota(jnp.int32, (radix_size, radix_size), 0)
    outer_col = lax.broadcasted_iota(jnp.int32, (radix_size, radix_size), 1)
    cosine, sine_table = phase_table(outer_row * outer_col % radix_size, radix_size)
    grouped = stacked.reshape(radix_size, inner_size, 2, width)
    grouped = jnp.transpose(grouped, (0, 2, 1, 3)).reshape(radix_size, 2 * inner_size * width)
    section = apply_stacked(cosine, sine_table, grouped, inner_size * width)
    section = section.reshape(radix_size, 2, inner_size, width)
    section_real = section[:, 0]
    section_imag = section[:, 1]
    twist_row = lax.broadcasted_iota(jnp.int32, (radix_size, inner_size, 1), 0)
    twist_col = lax.broadcasted_iota(jnp.int32, (radix_size, inner_size, 1), 1)
    twist_cos, twist_sin = phase_table(twist_row * twist_col, length)
    turned_real = section_real * twist_cos + section_imag * twist_sin
    turned_imag = section_imag * twist_cos - section_real * twist_sin
    turned = jnp.stack([turned_real, turned_imag], axis=0)
    turned = jnp.transpose(turned, (2, 0, 1, 3)).reshape(inner_size, 2 * radix_size * width)
    inner_row = lax.broadcasted_iota(jnp.int32, (inner_size, inner_size), 0)
    inner_col = lax.broadcasted_iota(jnp.int32, (inner_size, inner_size), 1)
    cosine2, sine_table2 = phase_table(inner_row * inner_col % inner_size, inner_size)
    final = apply_stacked(cosine2, sine_table2, turned, radix_size * width)
    final = final.reshape(inner_size, 2, radix_size, width)
    return jnp.transpose(final, (0, 2, 1, 3)).reshape(length, 2 * width)


def transform(columns):
    length, _, width = columns.shape
    stacked = columns.reshape(length, 2 * width)
    result = factored_transform(stacked, width)
    scale = 1.0 / jnp.sqrt(jnp.float32(length))
    return (result * scale).reshape(length, 2, width)


def on_device(visibilities, redundancy, mode_counts, filters):
    groups = lax.axis_size("tm")
    local_times, _, channels, raw_count = visibilities.shape
    uniques = filters.shape[4]
    kept = filters.shape[2]
    if fits(groups, local_times, channels, raw_count, uniques, kept):
        return fused_device(visibilities, redundancy, mode_counts, filters)
    unique_block = uniques // groups
    members = (
        redundancy[:, None] == lax.broadcasted_iota(jnp.int32, (raw_count, uniques), 1)
    ).astype(jnp.float32)
    weights = members / jnp.sum(members, axis=0, keepdims=True)
    flat_rows = visibilities.reshape(local_times, 2 * channels, raw_count)
    blocked_weights = weights.reshape(raw_count, groups, unique_block)
    packed = jnp.einsum(
        "tqr,rjc->tjqc",
        flat_rows,
        blocked_weights,
        precision=lax.Precision.HIGHEST,
        preferred_element_type=jnp.float32,
    )
    packed = packed.reshape(local_times, groups, 2 * channels * unique_block)
    arrived = lax.all_to_all(packed, "tm", split_axis=1, concat_axis=0, tiled=True)
    length = arrived.shape[0]
    spectra = transform(arrived.reshape(length, 2, channels * unique_block))
    spectra = spectra.reshape(length, 1, 2 * channels * unique_block)
    regrouped = lax.all_to_all(spectra, "tm", split_axis=0, concat_axis=1, tiled=True)
    regrouped = regrouped.reshape(local_times, groups, 2, channels, unique_block)
    mmodes = jnp.transpose(regrouped, (0, 2, 3, 1, 4)).reshape(local_times, 2, channels, uniques)
    local_modes = mmodes.shape[0]
    rounded = mmodes.astype(jnp.bfloat16).reshape(local_modes, 2, channels * uniques)
    flat_filters = filters.reshape(local_modes, 2, kept, channels * uniques)
    products = jnp.einsum(
        "mpkc,mqc->mpqk", flat_filters, rounded, preferred_element_type=jnp.float32
    )
    real_out = products[:, 0, 0] - products[:, 1, 1]
    imag_out = products[:, 0, 1] + products[:, 1, 0]
    kept_mask = lax.broadcasted_iota(jnp.int32, (local_modes, kept), 1) < mode_counts[:, None]
    modes = jnp.where(kept_mask[:, None, :], jnp.stack([real_out, imag_out], axis=1), 0.0)
    return (mmodes, modes)


def solution(mesh):
    return jax.shard_map(
        on_device,
        mesh=mesh,
        in_specs=(P("tm", None, "grp", None), P("grp"), P("tm"), P("tm", None, None, "grp", None)),
        out_specs=(P("tm", None, "grp", None), P("tm", None, "grp")),
        check_vma=False,
    )
```

```python
import functools

import numpy as np
import jax
import jax.numpy as jnp
from jax import lax
from jax.experimental import pallas as pl
from jax.experimental.pallas import tpu as pltpu
from jax.sharding import PartitionSpec as P

MESH = pl.DeviceIdType.MESH
LANES = 128
BLOCKS = 4
RADIX = 4
AHEAD = 3
GROUP = 16
NT = (((1,), (1,)), ((), ()))


def split_bf16(x):
    high = x.astype(jnp.bfloat16)
    return high, (x - high.astype(jnp.float32)).astype(jnp.bfloat16)


def rounded(x):
    return x.astype(jnp.bfloat16).astype(jnp.float32)[None]


def slab_factors(span, length):
    i = np.arange(span)
    side = np.sin(np.pi * (i[:-1] + 1) / length) * np.sin(np.pi * (span - 1 - i[:-1]) / length)
    middle = -np.cos(np.pi * (2 * i + 1 - span) / length) * np.cos(np.pi * span / length)
    _, basis = np.linalg.eigh(np.diag(middle) + np.diag(side, 1) + np.diag(side, -1))
    basis = basis[:, ::-1]
    mid = (span - 1) / 2
    at = i - mid
    basis = basis * np.where((1 + at / span) @ basis < 0, -1.0, 1.0)
    image = np.exp(-2j * np.pi / length * np.outer(at, at)) @ basis
    sizes = np.sqrt(np.sum(np.abs(image) ** 2, axis=0))
    rank = int(np.sum(sizes > sizes[0] * 2.0 ** -24))
    rank = -(-rank // 4) * 4
    dec = image[:, :rank] * np.exp(-2j * np.pi * mid / length * i)[:, None]
    enc = basis[:, :rank].T * np.exp(-2j * np.pi * mid / length * at)
    return dec, enc


def split_rows(rank):
    main = rank // 8 * 8
    return main, 2 * rank


def real_rows(re, im):
    main, _ = split_rows(re.shape[0])
    return np.concatenate([re[:main], im[:main], re[main:], im[main:]], axis=0)


def stacked_tables(slab, local):
    span = slab * local
    length = RADIX * span
    dec, enc = slab_factors(span, length)
    rank = enc.shape[0]
    rows = -(-2 * rank // 16) * 16
    deep = -(-2 * rank // LANES) * LANES
    per = local // RADIX
    bf16 = jnp.bfloat16

    def halves(a):
        high = a.astype(np.float32).astype(bf16)
        low = (a.astype(np.float32) - high.astype(np.float32)).astype(bf16)
        return np.concatenate([high, low], axis=0)

    enc_tables, dec_tables = [], []
    for r in range(RADIX):
        t = np.arange(span).reshape(slab, per, RADIX)[:, :, r]
        part = enc[:, t]
        cols = np.stack(
            [real_rows(part.real, part.imag), real_rows(-part.imag, part.real)], axis=2
        ).reshape(2 * rank, slab * 2 * per)
        enc_tables.append(halves(np.pad(cols, ((0, rows - 2 * rank), (0, 0)))))
        part = dec[t] * length ** -0.5
        part = np.moveaxis(part, -1, 0)
        cols = np.stack(
            [real_rows(part.real, -part.imag), real_rows(part.imag, part.real)], axis=2
        ).reshape(2 * rank, slab * 2 * per)
        dec_tables.append(halves(np.pad(cols, ((0, deep - 2 * rank), (0, 0))).T))
    return rank, jnp.asarray(np.stack(enc_tables)), jnp.asarray(np.stack(dec_tables))


def dft_radix(load, store, rank):
    main, total = split_rows(rank)

    def spread(g, turn):
        s02, d02 = g[0] + g[2], g[0] - g[2]
        s13, d13 = g[1] + g[3], turn(g[1] - g[3])
        return s02 + s13, d02 + d13, s02 - s13, d02 - d13

    def pair(q, carry):
        re = pl.ds(pl.multiple_of(q * 8, 8), 8)
        im = pl.ds(pl.multiple_of(main + q * 8, 8), 8)
        a = [load(k, re) for k in range(4)]
        b = [load(k, im) for k in range(4)]
        sa, da, sb, db = a[0] + a[2], a[0] - a[2], b[0] + b[2], b[0] - b[2]
        ta, ea, tb, eb = a[1] + a[3], a[1] - a[3], b[1] + b[3], b[1] - b[3]
        for k, (x, y) in enumerate(
            ((sa + ta, sb + tb), (da + eb, db - ea), (sa - ta, sb - tb), (da - eb, db + ea))
        ):
            store(k, re, x)
            store(k, im, y)
        return carry

    lax.fori_loop(0, main // 8, pair, 0, unroll=3)
    if total > 2 * main:
        at = pl.ds(2 * main, 8)
        sign = jnp.where(lax.broadcasted_iota(jnp.int32, (8, LANES), 0) < 4, 1.0, -1.0)
        out = spread([load(k, at) for k in range(4)], lambda v: pltpu.roll(v, 4, 0) * sign)
        for k in range(4):
            store(k, at, out[k])


def stacked_dot(table, x):
    high, low = split_bf16(x)
    out = jnp.dot(table, jnp.concatenate([high, low], axis=1), preferred_element_type=jnp.float32)
    out = out[:, :LANES] + out[:, LANES:]
    half = out.shape[0] // 2
    return out[:half] + out[half:]


def fused_kernel(
    n, local, chans, uniq, kept, rank,
    vis_ref, filt_ref, enc_hbm, dec_hbm, red_ref, counts_ref, mm_ref, modes_ref,
    send, recv, mix, send_b, recv_b, back, part, turned, enc, dec,
    load_sem, tab_sem, as_, ar, bs, br, cs, cr, filt_sem,
):
    slab = n // RADIX
    me = lax.axis_index("tm")
    z, c = lax.div(me, slab), lax.rem(me, slab)
    tiles = uniq // LANES
    per_dev = chans // slab
    steps = tiles * per_dev
    tb = local // BLOCKS
    vb = tb // RADIX
    per = local // RADIX
    width = 2 * chans
    total = 2 * rank

    table_copies = [
        pltpu.make_async_copy(enc_hbm, enc, tab_sem.at[0]),
        pltpu.make_async_copy(dec_hbm, dec, tab_sem.at[1]),
    ]
    def in_slab(o):
        return z * slab + lax.rem(c + o, slab)

    def across(o):
        return lax.rem(z + o, RADIX) * slab + c

    barrier = pltpu.get_barrier_semaphore()
    peers = [in_slab(o) for o in range(1, slab)] + [across(o) for o in range(1, RADIX)]
    odd = lax.rem(c, 2)
    near, ahead, behind = 1 + 2 * odd, 2 - odd, 3 - odd

    def slot(s):
        return lax.rem(s + steps, steps + 2)

    def remote(src, dst, ssem, rsem, peer):
        return pltpu.make_async_remote_copy(
            src_ref=src, dst_ref=dst, send_sem=ssem, recv_sem=rsem,
            device_id={"tm": peer}, device_id_type=MESH,
        )

    def first_part(i, o):
        at = pl.ds(i * vb if isinstance(i, int) else pl.multiple_of(i * vb, vb), vb)
        dest = lax.rem(c + o, slab)
        return remote(
            send.at[0, dest, :, :, at, :], recv.at[0, c, :, :, at, :],
            as_.at[0], ar.at[0], in_slab(o),
        )

    def first(s, o):
        dest = lax.rem(c + o, slab)
        return remote(send.at[s, dest], recv.at[s, c], as_.at[s], ar.at[s], in_slab(o))

    def second(s, o):
        dest = lax.rem(z + o, RADIX)
        return remote(send_b.at[s, dest], recv_b.at[s, z], bs, br.at[s], across(o))

    def all_first(s):
        some = pl.ds(0, slab - 1)
        return remote(send.at[s, some], recv.at[s, some], as_.at[s], ar.at[s], in_slab(1))

    def all_second(s):
        some = pl.ds(0, RADIX - 1)
        return remote(send_b.at[s, some], recv_b.at[s, some], bs, br.at[s], across(1))

    def all_third(s):
        some = pl.ds(0, slab - 1)
        return remote(send.at[s, some], recv.at[slot(s), some], cs, cr.at[s], in_slab(1))

    def last_third(blocks, late):
        s, some = steps - 1, pl.ds(0, blocks)
        return remote(send.at[s, some], recv.at[slot(s), some], cs, cr.at[s + late], in_slab(1))

    def third(s, o):
        dest = lax.rem(c + o, slab)
        far = lax.div(s, steps - 1) * (o != near).astype(jnp.int32)
        return remote(send.at[s, dest], recv.at[slot(s), c], cs, cr.at[s + far], in_slab(o))

    def encode(s):
        for r in range(RADIX):
            x = recv[s, :, r].reshape(slab * 2 * per, LANES)
            mix[r] = stacked_dot(enc[r], x)[:mix.shape[1]]

        def put(k, at, v):
            send_b[s, k, at, :] = v

        dft_radix(lambda k, at: mix[k, at, :], put, rank)
        recv_b[s, z] = send_b[s, z]
        for o in range(1, RADIX):
            second(s, o).start()

    def averages(vis_buf, wt, avg):
        def load(i, r):
            return pltpu.make_async_copy(
                vis_ref.at[pl.ds(i * vb, vb), r], vis_buf.at[i, r], load_sem.at[i]
            )

        for i in range(2):
            for r in range(RADIX):
                load(i, r).start()
        for peer in peers:
            pl.semaphore_signal(barrier, inc=1, device_id={"tm": peer}, device_id_type=MESH)
        wt[...] = (
            lax.broadcasted_iota(jnp.int32, wt.shape, 0) == red_ref[...]
        ).astype(jnp.float32).astype(jnp.bfloat16)
        ones = jnp.ones((8, wt.shape[1]), jnp.bfloat16)
        for i in range(2, BLOCKS):
            for r in range(RADIX):
                load(i, r).start()
        for copy in table_copies:
            copy.start()
        counts = lax.dot_general(ones, wt[...], NT, preferred_element_type=jnp.float32)
        inverse = 1.0 / counts[0:1]

        def average(i, h):
            at = pl.ds(i * vb if isinstance(i, int) else pl.multiple_of(i * vb, vb), vb)
            high, low = split_bf16(vis_buf[i].reshape(tb * width, vis_buf.shape[-1]))
            lanes = slice(h * 2 * LANES, (h + 1) * 2 * LANES)
            members = wt[lanes, :]
            summed = lax.dot_general(high, members, NT, preferred_element_type=jnp.float32)
            summed += lax.dot_general(low, members, NT, preferred_element_type=jnp.float32)
            mean = summed * inverse[:, lanes]
            for q in range(2):
                avg[q] = mean[:, q * LANES:(q + 1) * LANES]
            for q in range(2):
                for f in range(chans):
                    for r in range(RADIX):
                        for p in range(2):
                            s = (h * 2 + q) * per_dev + f % per_dev
                            send[s, f // per_dev, r, p, at, :] = avg[
                                q, pl.ds(r * vb * width + p * chans + f, vb, stride=width), :
                            ]

        def early(i, carry):
            pltpu.make_async_copy(vis_buf.at[i], vis_buf.at[i], load_sem.at[i]).wait()
            average(i, 0)

            @pl.when(i == 0)
            def _():
                pl.semaphore_wait(barrier, len(peers))

            first_part(i, near).start()
            first_part(i, ahead).start()
            return carry

        lax.fori_loop(0, BLOCKS, early, 0)
        for i in range(BLOCKS):
            first_part(i, behind).start()
        recv[0, c] = send[0, c]
        for copy in table_copies:
            copy.wait()
        all_first(0).wait_recv()
        for s in (1, 2):
            for o in range(1, slab):
                first(s, o).start()

        encode(0)

        def more(i, carry):
            average(i, 1)
            return carry

        lax.fori_loop(0, BLOCKS, more, 0)

    pl.run_scoped(
        averages,
        pltpu.VMEM((BLOCKS, RADIX, tb // RADIX, width, vis_ref.shape[-1]), jnp.float32),
        pltpu.VMEM((uniq, vis_ref.shape[-1]), jnp.bfloat16),
        pltpu.VMEM((2, tb * width, LANES), jnp.float32),
    )

    pl.run_scoped(
        functools.partial(
            transform_kernel, n, local, chans, uniq, kept, rank, filt_ref, counts_ref, mm_ref, modes_ref,
            send, recv, mix, send_b, recv_b, back, part, turned, enc, dec,
            first, second, third, all_first, all_second, all_third, last_third, encode, slot, filt_sem,
        ),
        pltpu.VMEM((tiles, local, 2, kept, chans, LANES), jnp.bfloat16),
    )


def transform_kernel(
    n, local, chans, uniq, kept, rank, filt_ref, counts_ref, mm_ref, modes_ref,
    send, recv, mix, send_b, recv_b, back, part, turned, enc, dec,
    first, second, third, all_first, all_second, all_third, last_third, encode, slot, filt_sem, filt,
):
    slab = n // RADIX
    me = lax.axis_index("tm")
    z, c = lax.div(me, slab), lax.rem(me, slab)
    tiles = uniq // LANES
    per_dev = chans // slab
    steps = tiles * per_dev
    per = local // RADIX
    width = 2 * chans
    total = 2 * rank
    stride = part.shape[0] // local

    def fetch(j):
        at = pl.multiple_of(j * LANES, LANES)
        return pltpu.make_async_copy(
            filt_ref.at[:, :, :, :, pl.ds(at, LANES)], filt.at[j], filt_sem.at[j]
        )

    for j in range(tiles):
        fetch(j).start()

    def keep(s, carry):
        recv[s, c] = send[s, c]
        return carry

    lax.fori_loop(1, steps, keep, 0)
    part[...] = jnp.zeros_like(part)
    def decode(s):
        all_second(s).wait_recv()

        def put(k, at, v):
            back[k, at, :] = v

        dft_radix(lambda k, at: recv_b[s, k, at, :], put, rank)
        for r in range(RADIX):
            y = stacked_dot(dec[r], back[r]).reshape(slab, 2, per, LANES)
            for d in range(slab):
                send[s, d, r] = y[d]
        recv[slot(s), c] = send[s, c]
        for o in range(1, slab):
            third(s, o).start()

    def place(s, j, f2):
        all_third(s).wait_recv()
        spread(s, j, f2, 0, slab)

    def spread(s, j, f2, low, high):
        def one(d, carry):
            for r in range(RADIX):
                for p in range(2):
                    start = (r * 2 + p) * chans + f2 + d * per_dev
                    mm_ref[j, pl.ds(start, per, stride=RADIX * width), :] = recv[slot(s), d, r, p]
            return carry

        lax.fori_loop(low, high, one, 0)

    def turn(j):
        fetch(j).wait()

        def one(m, carry):
            for p in range(2):
                turned[p] = filt[j, m, p].astype(jnp.float32).reshape(kept * chans, LANES)
            for p in range(2):
                for f in range(chans):
                    for g in range(kept // 8):
                        rows = turned[p, pl.ds(g * 8 * chans + f, 8, stride=chans), :]
                        filt[j, m, p, f * (kept // 8) + g] = rows.astype(jnp.bfloat16)
            return carry

        lax.fori_loop(0, local, one, 0)

    def project(j, f2, m, sources):
        per_chan = kept // 8
        re = pl.ds(pl.multiple_of(m * stride, 8), kept)
        im = pl.ds(pl.multiple_of(m * stride + kept, 8), kept)
        real, imag = part[re, :], part[im, :]
        for d in sources:
            f = d * per_dev + f2
            at = f * per_chan
            x0 = mm_ref[j, pl.ds(m * width + f, 1), :].astype(jnp.bfloat16).astype(jnp.float32)
            x1 = mm_ref[j, pl.ds(m * width + chans + f, 1), :].astype(jnp.bfloat16).astype(jnp.float32)
            f0 = filt[j, m, 0, pl.ds(at, per_chan)].astype(jnp.float32).reshape(kept, LANES)
            f1 = filt[j, m, 1, pl.ds(at, per_chan)].astype(jnp.float32).reshape(kept, LANES)
            real += f0 * x0 - f1 * x1
            imag += f0 * x1 + f1 * x0
        part[re, :] = real
        part[im, :] = imag

    def projects(j, f2, sources):
        def one(m, carry):
            project(j, f2, m, sources)
            return carry

        lax.fori_loop(0, local, one, 0, unroll=2)

    back[:, total:, :] = jnp.zeros((RADIX, back.shape[1] - total, LANES), jnp.float32)

    def later(e):
        all_first(e).wait_recv()

        @pl.when(e + 2 < steps)
        def _():
            for o in range(1, slab):
                first(e + 2, o).start()

        encode(e)

    for e in range(1, AHEAD):
        later(e)

    turn(0)

    def step(d, carry):
        @pl.when((d == 1) | (d == 2))
        def _():
            turn(d)

        @pl.when(d == 1)
        def _():
            turn(tiles - 1)

        @pl.when(d >= 2)
        def _():
            j, f2 = lax.div(d - 2, per_dev), lax.rem(d - 2, per_dev)
            place(d - 2, j, f2)

            projects(j, f2, range(slab))

        all_first(d).wait_send()
        decode(d)

        @pl.when(d + AHEAD < steps)
        def _():
            later(d + AHEAD)

        return carry

    lax.fori_loop(0, steps, step, 0)

    j = tiles - 1
    lane = lax.broadcasted_iota(jnp.int32, (kept, LANES), 1)

    def gather(q, outs):
        outs = list(outs)
        for i in range(GROUP):
            m = q * GROUP + i
            for p in range(2):
                at = pl.ds(pl.multiple_of(m * stride + p * kept, 8), kept)
                row = jnp.sum(part[at, :], axis=1, keepdims=True)
                outs[p] = jnp.where(lane == m, row, outs[p])
        return tuple(outs)

    for f2 in range(per_dev - 1):
        place(j * per_dev + f2, j, f2)
        projects(j, f2, range(slab))
    f2 = per_dev - 1
    half = slab // 2
    order = lax.broadcasted_iota(jnp.int32, (kept, LANES), 0)
    zero = jnp.zeros((kept, LANES), jnp.float32)

    def finish(early, late):
        last_third(1, 0).wait_recv()
        spread(steps - 1, j, f2, early[0], early[0] + half)
        projects(j, f2, early)
        last_third(2, 1).wait_recv()
        spread(steps - 1, j, f2, late[0], late[0] + half)

        def last(q, outs):
            outs = gather(jnp.maximum(q - 1, 0), outs)
            for i in range(GROUP):
                project(j, f2, q * GROUP + i, late)
            return outs

        outs = lax.fori_loop(0, local // GROUP, last, (zero, zero))
        outs = gather(local // GROUP - 1, outs)
        for p in range(2):
            modes_ref[p] = jnp.where(order < counts_ref[...], outs[p], 0.0)

    @pl.when(lax.div(c, half) == 0)
    def _():
        finish(range(half), range(half, slab))

    @pl.when(lax.div(c, half) == 1)
    def _():
        finish(range(half, slab), range(half))

    def drain(s, carry):
        all_second(s).wait_send()
        all_third(s).wait_send()
        return carry

    lax.fori_loop(0, steps, drain, 0)


def emit_kernel(mm_ref, modes_ref, out_ref, kept_ref, out_sem):
    tiles, chunks = out_sem.shape
    rows = mm_ref.shape[1] // chunks

    def write(t, q):
        at = pl.ds(q * rows, rows)
        return pltpu.make_async_copy(
            mm_ref.at[t, at], out_ref.at[at, pl.ds(t * LANES, LANES)], out_sem.at[t, q]
        )

    for t in range(tiles):
        for q in range(chunks):
            write(t, q).start()
    kept_ref[...] = modes_ref[...]
    for t in range(tiles):
        for q in range(chunks):
            write(t, q).wait()


def fits(n, local, chans, raw, uniq, kept):
    slab = n // RADIX
    return (
        n == RADIX * slab
        and slab == 4
        and chans == 8
        and chans % slab == 0
        and local % (BLOCKS * RADIX * 8) == 0
        and slab * local * 2 // RADIX <= 2 * LANES
        and raw % LANES == 0
        and raw <= 8 * LANES
        and uniq % LANES == 0
        and uniq == 4 * LANES
        and local == LANES
        and kept == 16
        and chans // slab == 2
    )


def fused_device(visibilities, redundancy, mode_counts, filters):
    n = lax.axis_size("tm")
    local, _, chans, raw = visibilities.shape
    uniq, kept = filters.shape[4], filters.shape[2]
    slab = n // RADIX
    tiles = uniq // LANES
    per_dev = chans // slab
    steps = tiles * per_dev
    per = local // RADIX
    width = 2 * chans
    rank, enc, dec = stacked_tables(slab, local)
    total = 2 * rank
    vmem = pl.BlockSpec(memory_space=pltpu.VMEM)
    hbm = pl.BlockSpec(memory_space=pl.ANY)
    f32, bf16 = jnp.float32, jnp.bfloat16
    dma = pltpu.SemaphoreType.DMA
    stride = 2 * kept
    mm, modes = pl.pallas_call(
        functools.partial(fused_kernel, n, local, chans, uniq, kept, rank),
        out_shape=(
            pltpu.VMEM((tiles, local * width, LANES), f32),
            pltpu.VMEM((2, kept, local), f32),
        ),
        in_specs=[hbm] * 4 + [vmem] * 2,
        out_specs=(pl.BlockSpec(memory_space=pltpu.VMEM), vmem),
        scratch_shapes=[
            pltpu.VMEM((steps, slab, RADIX, 2, per, LANES), f32),
            pltpu.VMEM((steps + 2, slab, RADIX, 2, per, LANES), f32),
            pltpu.VMEM((RADIX, total, LANES), f32),
            pltpu.VMEM((steps, RADIX, total, LANES), f32),
            pltpu.VMEM((steps, RADIX, total, LANES), f32),
            pltpu.VMEM((RADIX, dec.shape[2], LANES), f32),
            pltpu.VMEM((local * stride, LANES), f32),
            pltpu.VMEM((2, kept * chans, LANES), f32),
            pltpu.VMEM(enc.shape, bf16),
            pltpu.VMEM(dec.shape, bf16),
            dma((BLOCKS,)),
            dma((2,)),
            dma((steps,)),
            dma((steps,)),
            dma,
            dma((steps,)),
            dma,
            dma((steps + 1,)),
            dma((tiles,)),
        ],
        compiler_params=pltpu.CompilerParams(
            collective_id=0, has_side_effects=True, vmem_limit_bytes=62_700_000
        ),
        name="fused",
    )(
        visibilities.reshape(local // RADIX, RADIX, width, raw),
        filters, enc, dec, redundancy.reshape(1, raw), mode_counts.reshape(1, local),
    )
    chunks = 8
    mmodes, modes = pl.pallas_call(
        emit_kernel,
        out_shape=(
            jax.ShapeDtypeStruct((local * width, uniq), f32),
            jax.ShapeDtypeStruct((2, kept, local), f32),
        ),
        in_specs=[vmem, vmem],
        out_specs=(hbm, vmem),
        scratch_shapes=[dma((tiles, chunks))],
        compiler_params=pltpu.CompilerParams(vmem_limit_bytes=32 * 2**20),
        name="emit",
    )(mm, modes)
    return mmodes.reshape(local, 2, chans, uniq), jnp.transpose(modes, (2, 0, 1))


def phase_table(numer, period):
    phases = 2.0 * jnp.pi / period * numer.astype(jnp.float32)
    return (jnp.cos(phases), jnp.sin(phases))


def apply_stacked(cosine, sine_table, stacked, width):
    cos_part = jnp.dot(
        cosine, stacked, precision=lax.Precision.HIGHEST, preferred_element_type=jnp.float32
    )
    sin_part = jnp.dot(
        sine_table, stacked, precision=lax.Precision.HIGHEST, preferred_element_type=jnp.float32
    )
    real_out = cos_part[:, :width] + sin_part[:, width:]
    imag_out = cos_part[:, width:] - sin_part[:, :width]
    return jnp.concatenate([real_out, imag_out], axis=1)


def factored_transform(stacked, width):
    length = stacked.shape[0]
    radix_size = 64
    inner_size = length // radix_size
    outer_row = lax.broadcasted_iota(jnp.int32, (radix_size, radix_size), 0)
    outer_col = lax.broadcasted_iota(jnp.int32, (radix_size, radix_size), 1)
    cosine, sine_table = phase_table(outer_row * outer_col % radix_size, radix_size)
    grouped = stacked.reshape(radix_size, inner_size, 2, width)
    grouped = jnp.transpose(grouped, (0, 2, 1, 3)).reshape(radix_size, 2 * inner_size * width)
    section = apply_stacked(cosine, sine_table, grouped, inner_size * width)
    section = section.reshape(radix_size, 2, inner_size, width)
    section_real = section[:, 0]
    section_imag = section[:, 1]
    twist_row = lax.broadcasted_iota(jnp.int32, (radix_size, inner_size, 1), 0)
    twist_col = lax.broadcasted_iota(jnp.int32, (radix_size, inner_size, 1), 1)
    twist_cos, twist_sin = phase_table(twist_row * twist_col, length)
    turned_real = section_real * twist_cos + section_imag * twist_sin
    turned_imag = section_imag * twist_cos - section_real * twist_sin
    turned = jnp.stack([turned_real, turned_imag], axis=0)
    turned = jnp.transpose(turned, (2, 0, 1, 3)).reshape(inner_size, 2 * radix_size * width)
    inner_row = lax.broadcasted_iota(jnp.int32, (inner_size, inner_size), 0)
    inner_col = lax.broadcasted_iota(jnp.int32, (inner_size, inner_size), 1)
    cosine2, sine_table2 = phase_table(inner_row * inner_col % inner_size, inner_size)
    final = apply_stacked(cosine2, sine_table2, turned, radix_size * width)
    final = final.reshape(inner_size, 2, radix_size, width)
    return jnp.transpose(final, (0, 2, 1, 3)).reshape(length, 2 * width)


def transform(columns):
    length, _, width = columns.shape
    stacked = columns.reshape(length, 2 * width)
    result = factored_transform(stacked, width)
    scale = 1.0 / jnp.sqrt(jnp.float32(length))
    return (result * scale).reshape(length, 2, width)


def on_device(visibilities, redundancy, mode_counts, filters):
    groups = lax.axis_size("tm")
    local_times, _, channels, raw_count = visibilities.shape
    uniques = filters.shape[4]
    kept = filters.shape[2]
    if fits(groups, local_times, channels, raw_count, uniques, kept):
        return fused_device(visibilities, redundancy, mode_counts, filters)
    unique_block = uniques // groups
    members = (
        redundancy[:, None] == lax.broadcasted_iota(jnp.int32, (raw_count, uniques), 1)
    ).astype(jnp.float32)
    weights = members / jnp.sum(members, axis=0, keepdims=True)
    flat_rows = visibilities.reshape(local_times, 2 * channels, raw_count)
    blocked_weights = weights.reshape(raw_count, groups, unique_block)
    packed = jnp.einsum(
        "tqr,rjc->tjqc",
        flat_rows,
        blocked_weights,
        precision=lax.Precision.HIGHEST,
        preferred_element_type=jnp.float32,
    )
    packed = packed.reshape(local_times, groups, 2 * channels * unique_block)
    arrived = lax.all_to_all(packed, "tm", split_axis=1, concat_axis=0, tiled=True)
    length = arrived.shape[0]
    spectra = transform(arrived.reshape(length, 2, channels * unique_block))
    spectra = spectra.reshape(length, 1, 2 * channels * unique_block)
    regrouped = lax.all_to_all(spectra, "tm", split_axis=0, concat_axis=1, tiled=True)
    regrouped = regrouped.reshape(local_times, groups, 2, channels, unique_block)
    mmodes = jnp.transpose(regrouped, (0, 2, 3, 1, 4)).reshape(local_times, 2, channels, uniques)
    local_modes = mmodes.shape[0]
    rounded = mmodes.astype(jnp.bfloat16).reshape(local_modes, 2, channels * uniques)
    flat_filters = filters.reshape(local_modes, 2, kept, channels * uniques)
    products = jnp.einsum(
        "mpkc,mqc->mpqk", flat_filters, rounded, preferred_element_type=jnp.float32
    )
    real_out = products[:, 0, 0] - products[:, 1, 1]
    imag_out = products[:, 0, 1] + products[:, 1, 0]
    kept_mask = lax.broadcasted_iota(jnp.int32, (local_modes, kept), 1) < mode_counts[:, None]
    modes = jnp.where(kept_mask[:, None, :], jnp.stack([real_out, imag_out], axis=1), 0.0)
    return (mmodes, modes)


def solution(mesh):
    return jax.shard_map(
        on_device,
        mesh=mesh,
        in_specs=(P("tm", None, "grp", None), P("grp"), P("tm"), P("tm", None, None, "grp", None)),
        out_specs=(P("tm", None, "grp", None), P("tm", None, "grp")),
        check_vma=False,
    )
```

```python
import functools

import numpy as np
import jax
import jax.numpy as jnp
from jax import lax
from jax.experimental import pallas as pl
from jax.experimental.pallas import tpu as pltpu
from jax.sharding import PartitionSpec as P

MESH = pl.DeviceIdType.MESH
LANES = 128
BLOCKS = 4
RADIX = 4
AHEAD = 3
GROUP = 16
NT = (((1,), (1,)), ((), ()))


def split_bf16(x):
    high = x.astype(jnp.bfloat16)
    return high, (x - high.astype(jnp.float32)).astype(jnp.bfloat16)


def rounded(x):
    return x.astype(jnp.bfloat16).astype(jnp.float32)[None]


def slab_factors(span, length):
    i = np.arange(span)
    side = np.sin(np.pi * (i[:-1] + 1) / length) * np.sin(np.pi * (span - 1 - i[:-1]) / length)
    middle = -np.cos(np.pi * (2 * i + 1 - span) / length) * np.cos(np.pi * span / length)
    _, basis = np.linalg.eigh(np.diag(middle) + np.diag(side, 1) + np.diag(side, -1))
    basis = basis[:, ::-1]
    mid = (span - 1) / 2
    at = i - mid
    basis = basis * np.where((1 + at / span) @ basis < 0, -1.0, 1.0)
    image = np.exp(-2j * np.pi / length * np.outer(at, at)) @ basis
    sizes = np.sqrt(np.sum(np.abs(image) ** 2, axis=0))
    rank = int(np.sum(sizes > sizes[0] * 2.0 ** -24))
    rank = -(-rank // 4) * 4
    dec = image[:, :rank] * np.exp(-2j * np.pi * mid / length * i)[:, None]
    enc = basis[:, :rank].T * np.exp(-2j * np.pi * mid / length * at)
    return dec, enc


def split_rows(rank):
    main = rank // 8 * 8
    return main, 2 * rank


def real_rows(re, im):
    main, _ = split_rows(re.shape[0])
    return np.concatenate([re[:main], im[:main], re[main:], im[main:]], axis=0)


def stacked_tables(slab, local):
    span = slab * local
    length = RADIX * span
    dec, enc = slab_factors(span, length)
    rank = enc.shape[0]
    rows = -(-2 * rank // 16) * 16
    deep = -(-2 * rank // LANES) * LANES
    per = local // RADIX
    bf16 = jnp.bfloat16

    def halves(a):
        high = a.astype(np.float32).astype(bf16)
        low = (a.astype(np.float32) - high.astype(np.float32)).astype(bf16)
        return np.concatenate([high, low], axis=0)

    enc_tables, dec_tables = [], []
    for r in range(RADIX):
        t = np.arange(span).reshape(slab, per, RADIX)[:, :, r]
        part = enc[:, t]
        cols = np.stack(
            [real_rows(part.real, part.imag), real_rows(-part.imag, part.real)], axis=2
        ).reshape(2 * rank, slab * 2 * per)
        enc_tables.append(halves(np.pad(cols, ((0, rows - 2 * rank), (0, 0)))))
        part = dec[t] * length ** -0.5
        part = np.moveaxis(part, -1, 0)
        cols = np.stack(
            [real_rows(part.real, -part.imag), real_rows(part.imag, part.real)], axis=2
        ).reshape(2 * rank, slab * 2 * per)
        dec_tables.append(halves(np.pad(cols, ((0, deep - 2 * rank), (0, 0))).T))
    return rank, jnp.asarray(np.stack(enc_tables)), jnp.asarray(np.stack(dec_tables))


def dft_radix(load, store, rank):
    main, total = split_rows(rank)

    def spread(g, turn):
        s02, d02 = g[0] + g[2], g[0] - g[2]
        s13, d13 = g[1] + g[3], turn(g[1] - g[3])
        return s02 + s13, d02 + d13, s02 - s13, d02 - d13

    def pair(q, carry):
        re = pl.ds(pl.multiple_of(q * 8, 8), 8)
        im = pl.ds(pl.multiple_of(main + q * 8, 8), 8)
        a = [load(k, re) for k in range(4)]
        b = [load(k, im) for k in range(4)]
        sa, da, sb, db = a[0] + a[2], a[0] - a[2], b[0] + b[2], b[0] - b[2]
        ta, ea, tb, eb = a[1] + a[3], a[1] - a[3], b[1] + b[3], b[1] - b[3]
        for k, (x, y) in enumerate(
            ((sa + ta, sb + tb), (da + eb, db - ea), (sa - ta, sb - tb), (da - eb, db + ea))
        ):
            store(k, re, x)
            store(k, im, y)
        return carry

    lax.fori_loop(0, main // 8, pair, 0, unroll=3)
    if total > 2 * main:
        at = pl.ds(2 * main, 8)
        sign = jnp.where(lax.broadcasted_iota(jnp.int32, (8, LANES), 0) < 4, 1.0, -1.0)
        out = spread([load(k, at) for k in range(4)], lambda v: pltpu.roll(v, 4, 0) * sign)
        for k in range(4):
            store(k, at, out[k])


def stacked_dot(table, x):
    high, low = split_bf16(x)
    out = jnp.dot(table, jnp.concatenate([high, low], axis=1), preferred_element_type=jnp.float32)
    out = out[:, :LANES] + out[:, LANES:]
    half = out.shape[0] // 2
    return out[:half] + out[half:]


def fused_kernel(
    n, local, chans, uniq, kept, rank,
    vis_ref, filt_ref, enc_hbm, dec_hbm, red_ref, counts_ref, mm_ref, modes_ref,
    send, recv, mix, send_b, recv_b, back, part, turned, enc, dec,
    load_sem, tab_sem, as_, ar, bs, br, cs, cr, filt_sem,
):
    slab = n // RADIX
    me = lax.axis_index("tm")
    z, c = lax.div(me, slab), lax.rem(me, slab)
    tiles = uniq // LANES
    per_dev = chans // slab
    steps = tiles * per_dev
    tb = local // BLOCKS
    vb = tb // RADIX
    per = local // RADIX
    width = 2 * chans
    total = 2 * rank

    table_copies = [
        pltpu.make_async_copy(enc_hbm, enc, tab_sem.at[0]),
        pltpu.make_async_copy(dec_hbm, dec, tab_sem.at[1]),
    ]
    def in_slab(o):
        return z * slab + lax.rem(c + o, slab)

    def across(o):
        return lax.rem(z + o, RADIX) * slab + c

    barrier = pltpu.get_barrier_semaphore()
    peers = [in_slab(o) for o in range(1, slab)] + [across(o) for o in range(1, RADIX)]
    odd = lax.rem(c, 2)
    near, ahead, behind = 1 + 2 * odd, 2 - odd, 3 - odd

    def slot(s):
        return lax.rem(s + steps, steps + 2)

    def remote(src, dst, ssem, rsem, peer):
        return pltpu.make_async_remote_copy(
            src_ref=src, dst_ref=dst, send_sem=ssem, recv_sem=rsem,
            device_id={"tm": peer}, device_id_type=MESH,
        )

    def first_part(i, o):
        at = pl.ds(i * vb if isinstance(i, int) else pl.multiple_of(i * vb, vb), vb)
        dest = lax.rem(c + o, slab)
        return remote(
            send.at[0, dest, :, :, at, :], recv.at[0, c, :, :, at, :],
            as_.at[0], ar.at[0], in_slab(o),
        )

    def first(s, o):
        dest = lax.rem(c + o, slab)
        return remote(send.at[s, dest], recv.at[s, c], as_.at[s], ar.at[s], in_slab(o))

    def second(s, o):
        dest = lax.rem(z + o, RADIX)
        return remote(send_b.at[s, dest], recv_b.at[s, z], bs, br.at[s], across(o))

    def all_first(s):
        some = pl.ds(0, slab - 1)
        return remote(send.at[s, some], recv.at[s, some], as_.at[s], ar.at[s], in_slab(1))

    def all_second(s):
        some = pl.ds(0, RADIX - 1)
        return remote(send_b.at[s, some], recv_b.at[s, some], bs, br.at[s], across(1))

    def all_third(s):
        some = pl.ds(0, slab - 1)
        return remote(send.at[s, some], recv.at[slot(s), some], cs, cr.at[s], in_slab(1))

    def last_third(blocks, late):
        s, some = steps - 1, pl.ds(0, blocks)
        return remote(send.at[s, some], recv.at[slot(s), some], cs, cr.at[s + late], in_slab(1))

    def third(s, o):
        dest = lax.rem(c + o, slab)
        far = lax.div(s, steps - 1) * (o != near).astype(jnp.int32)
        return remote(send.at[s, dest], recv.at[slot(s), c], cs, cr.at[s + far], in_slab(o))

    def encode(s):
        for r in range(RADIX):
            x = recv[s, :, r].reshape(slab * 2 * per, LANES)
            mix[r] = stacked_dot(enc[r], x)[:mix.shape[1]]

        def put(k, at, v):
            send_b[s, k, at, :] = v

        dft_radix(lambda k, at: mix[k, at, :], put, rank)
        recv_b[s, z] = send_b[s, z]
        for o in range(1, RADIX):
            second(s, o).start()

    def averages(vis_buf, wt, avg):
        def load(i, r):
            return pltpu.make_async_copy(
                vis_ref.at[pl.ds(i * vb, vb), r], vis_buf.at[i, r], load_sem.at[i]
            )

        for r in range(RADIX):
            load(0, r).start()
        for peer in peers:
            pl.semaphore_signal(barrier, inc=1, device_id={"tm": peer}, device_id_type=MESH)
        def members_of(h):
            rows = slice(h * 2 * LANES, (h + 1) * 2 * LANES)
            shape = (2 * LANES, wt.shape[1])
            wt[rows, :] = (
                lax.broadcasted_iota(jnp.int32, shape, 0) + h * 2 * LANES == red_ref[...]
            ).astype(jnp.float32).astype(jnp.bfloat16)

        def inverse_of(h):
            rows = slice(h * 2 * LANES, (h + 1) * 2 * LANES)
            ones = jnp.ones((8, wt.shape[1]), jnp.bfloat16)
            counts = lax.dot_general(ones, wt[rows, :], NT, preferred_element_type=jnp.float32)
            return 1.0 / counts[0:1]

        members_of(0)
        for r in range(RADIX):
            load(1, r).start()
        inverse = inverse_of(0)

        def average(i, h, inverse):
            at = pl.ds(i * vb if isinstance(i, int) else pl.multiple_of(i * vb, vb), vb)
            high, low = split_bf16(vis_buf[i].reshape(tb * width, vis_buf.shape[-1]))
            lanes = slice(h * 2 * LANES, (h + 1) * 2 * LANES)
            members = wt[lanes, :]
            summed = lax.dot_general(high, members, NT, preferred_element_type=jnp.float32)
            summed += lax.dot_general(low, members, NT, preferred_element_type=jnp.float32)
            mean = summed * inverse
            for q in range(2):
                avg[q] = mean[:, q * LANES:(q + 1) * LANES]
            for q in range(2):
                for f in range(chans):
                    for r in range(RADIX):
                        for p in range(2):
                            s = (h * 2 + q) * per_dev + f % per_dev
                            send[s, f // per_dev, r, p, at, :] = avg[
                                q, pl.ds(r * vb * width + p * chans + f, vb, stride=width), :
                            ]

        def early(i, carry):
            pltpu.make_async_copy(vis_buf.at[i], vis_buf.at[i], load_sem.at[i]).wait()
            @pl.when(i + 2 < BLOCKS)
            def _():
                for r in range(RADIX):
                    load(i + 2, r).start()

            average(i, 0, inverse)

            @pl.when(i == 0)
            def _():
                pl.semaphore_wait(barrier, len(peers))

            first_part(i, near).start()
            first_part(i, ahead).start()
            return carry

        lax.fori_loop(0, BLOCKS, early, 0)
        for copy in table_copies:
            copy.start()
        for i in range(BLOCKS):
            first_part(i, behind).start()
        recv[0, c] = send[0, c]
        for copy in table_copies:
            copy.wait()
        all_first(0).wait_recv()
        for s in (1, 2):
            for o in range(1, slab):
                first(s, o).start()

        encode(0)

        members_of(1)
        inverse_rest = inverse_of(1)

        def more(i, carry):
            average(i, 1, inverse_rest)
            return carry

        lax.fori_loop(0, BLOCKS, more, 0)

    pl.run_scoped(
        averages,
        pltpu.VMEM((BLOCKS, RADIX, tb // RADIX, width, vis_ref.shape[-1]), jnp.float32),
        pltpu.VMEM((uniq, vis_ref.shape[-1]), jnp.bfloat16),
        pltpu.VMEM((2, tb * width, LANES), jnp.float32),
    )

    pl.run_scoped(
        functools.partial(
            transform_kernel, n, local, chans, uniq, kept, rank, filt_ref, counts_ref, mm_ref, modes_ref,
            send, recv, mix, send_b, recv_b, back, part, turned, enc, dec,
            first, second, third, all_first, all_second, all_third, last_third, encode, slot, filt_sem,
        ),
        pltpu.VMEM((tiles, local, 2, kept, chans, LANES), jnp.bfloat16),
    )


def transform_kernel(
    n, local, chans, uniq, kept, rank, filt_ref, counts_ref, mm_ref, modes_ref,
    send, recv, mix, send_b, recv_b, back, part, turned, enc, dec,
    first, second, third, all_first, all_second, all_third, last_third, encode, slot, filt_sem, filt,
):
    slab = n // RADIX
    me = lax.axis_index("tm")
    z, c = lax.div(me, slab), lax.rem(me, slab)
    tiles = uniq // LANES
    per_dev = chans // slab
    steps = tiles * per_dev
    per = local // RADIX
    width = 2 * chans
    total = 2 * rank
    stride = part.shape[0] // local

    def fetch(j):
        at = pl.multiple_of(j * LANES, LANES)
        return pltpu.make_async_copy(
            filt_ref.at[:, :, :, :, pl.ds(at, LANES)], filt.at[j], filt_sem.at[j]
        )

    for j in range(tiles):
        fetch(j).start()

    def keep(s, carry):
        recv[s, c] = send[s, c]
        return carry

    lax.fori_loop(1, steps, keep, 0)
    part[...] = jnp.zeros_like(part)
    def decode(s):
        all_second(s).wait_recv()

        def put(k, at, v):
            back[k, at, :] = v

        dft_radix(lambda k, at: recv_b[s, k, at, :], put, rank)
        for r in range(RADIX):
            y = stacked_dot(dec[r], back[r]).reshape(slab, 2, per, LANES)
            for d in range(slab):
                send[s, d, r] = y[d]
        recv[slot(s), c] = send[s, c]
        for o in range(1, slab):
            third(s, o).start()

    def place(s, j, f2):
        all_third(s).wait_recv()
        spread(s, j, f2, 0, slab)

    def spread(s, j, f2, low, high):
        def one(d, carry):
            for r in range(RADIX):
                for p in range(2):
                    start = (r * 2 + p) * chans + f2 + d * per_dev
                    mm_ref[j, pl.ds(start, per, stride=RADIX * width), :] = recv[slot(s), d, r, p]
            return carry

        lax.fori_loop(low, high, one, 0)

    def turn(j):
        fetch(j).wait()

        def one(m, carry):
            for p in range(2):
                turned[p] = filt[j, m, p].astype(jnp.float32).reshape(kept * chans, LANES)
            for p in range(2):
                for f in range(chans):
                    for g in range(kept // 8):
                        rows = turned[p, pl.ds(g * 8 * chans + f, 8, stride=chans), :]
                        filt[j, m, p, f * (kept // 8) + g] = rows.astype(jnp.bfloat16)
            return carry

        lax.fori_loop(0, local, one, 0)

    def project(j, f2, m, sources):
        per_chan = kept // 8
        re = pl.ds(pl.multiple_of(m * stride, 8), kept)
        im = pl.ds(pl.multiple_of(m * stride + kept, 8), kept)
        real, imag = part[re, :], part[im, :]
        for d in sources:
            f = d * per_dev + f2
            at = f * per_chan
            x0 = mm_ref[j, pl.ds(m * width + f, 1), :].astype(jnp.bfloat16).astype(jnp.float32)
            x1 = mm_ref[j, pl.ds(m * width + chans + f, 1), :].astype(jnp.bfloat16).astype(jnp.float32)
            f0 = filt[j, m, 0, pl.ds(at, per_chan)].astype(jnp.float32).reshape(kept, LANES)
            f1 = filt[j, m, 1, pl.ds(at, per_chan)].astype(jnp.float32).reshape(kept, LANES)
            real += f0 * x0 - f1 * x1
            imag += f0 * x1 + f1 * x0
        part[re, :] = real
        part[im, :] = imag

    def projects(j, f2, sources):
        def one(m, carry):
            project(j, f2, m, sources)
            return carry

        lax.fori_loop(0, local, one, 0, unroll=2)

    back[:, total:, :] = jnp.zeros((RADIX, back.shape[1] - total, LANES), jnp.float32)

    def later(e):
        all_first(e).wait_recv()

        @pl.when(e + 2 < steps)
        def _():
            for o in range(1, slab):
                first(e + 2, o).start()

        encode(e)

    for e in range(1, AHEAD):
        later(e)

    turn(0)

    def step(d, carry):
        @pl.when((d == 1) | (d == 2))
        def _():
            turn(d)

        @pl.when(d == 1)
        def _():
            turn(tiles - 1)

        @pl.when(d >= 2)
        def _():
            j, f2 = lax.div(d - 2, per_dev), lax.rem(d - 2, per_dev)
            place(d - 2, j, f2)

            projects(j, f2, range(slab))

        all_first(d).wait_send()
        decode(d)

        @pl.when(d + AHEAD < steps)
        def _():
            later(d + AHEAD)

        return carry

    lax.fori_loop(0, steps, step, 0)

    j = tiles - 1
    lane = lax.broadcasted_iota(jnp.int32, (kept, LANES), 1)

    def gather(q, outs):
        outs = list(outs)
        for i in range(GROUP):
            m = q * GROUP + i
            for p in range(2):
                at = pl.ds(pl.multiple_of(m * stride + p * kept, 8), kept)
                row = jnp.sum(part[at, :], axis=1, keepdims=True)
                outs[p] = jnp.where(lane == m, row, outs[p])
        return tuple(outs)

    for f2 in range(per_dev - 1):
        place(j * per_dev + f2, j, f2)
        projects(j, f2, range(slab))
    f2 = per_dev - 1
    half = slab // 2
    order = lax.broadcasted_iota(jnp.int32, (kept, LANES), 0)
    zero = jnp.zeros((kept, LANES), jnp.float32)

    def finish(early, late):
        last_third(1, 0).wait_recv()
        spread(steps - 1, j, f2, early[0], early[0] + half)
        projects(j, f2, early)
        last_third(2, 1).wait_recv()
        spread(steps - 1, j, f2, late[0], late[0] + half)

        def last(q, outs):
            outs = gather(jnp.maximum(q - 1, 0), outs)
            for i in range(GROUP):
                project(j, f2, q * GROUP + i, late)
            return outs

        outs = lax.fori_loop(0, local // GROUP, last, (zero, zero))
        outs = gather(local // GROUP - 1, outs)
        for p in range(2):
            modes_ref[p] = jnp.where(order < counts_ref[...], outs[p], 0.0)

    @pl.when(lax.div(c, half) == 0)
    def _():
        finish(range(half), range(half, slab))

    @pl.when(lax.div(c, half) == 1)
    def _():
        finish(range(half, slab), range(half))

    def drain(s, carry):
        all_second(s).wait_send()
        all_third(s).wait_send()
        return carry

    lax.fori_loop(0, steps, drain, 0)


def emit_kernel(mm_ref, modes_ref, out_ref, kept_ref, out_sem):
    tiles, chunks = out_sem.shape
    rows = mm_ref.shape[1] // chunks

    def write(t, q):
        at = pl.ds(q * rows, rows)
        return pltpu.make_async_copy(
            mm_ref.at[t, at], out_ref.at[at, pl.ds(t * LANES, LANES)], out_sem.at[t, q]
        )

    for t in range(tiles):
        for q in range(chunks):
            write(t, q).start()
    kept_ref[...] = modes_ref[...]
    for t in range(tiles):
        for q in range(chunks):
            write(t, q).wait()


def fits(n, local, chans, raw, uniq, kept):
    slab = n // RADIX
    return (
        n == RADIX * slab
        and slab == 4
        and chans == 8
        and chans % slab == 0
        and local % (BLOCKS * RADIX * 8) == 0
        and slab * local * 2 // RADIX <= 2 * LANES
        and raw % LANES == 0
        and raw <= 8 * LANES
        and uniq % LANES == 0
        and uniq == 4 * LANES
        and local == LANES
        and kept == 16
        and chans // slab == 2
    )


def fused_device(visibilities, redundancy, mode_counts, filters):
    n = lax.axis_size("tm")
    local, _, chans, raw = visibilities.shape
    uniq, kept = filters.shape[4], filters.shape[2]
    slab = n // RADIX
    tiles = uniq // LANES
    per_dev = chans // slab
    steps = tiles * per_dev
    per = local // RADIX
    width = 2 * chans
    rank, enc, dec = stacked_tables(slab, local)
    total = 2 * rank
    vmem = pl.BlockSpec(memory_space=pltpu.VMEM)
    hbm = pl.BlockSpec(memory_space=pl.ANY)
    f32, bf16 = jnp.float32, jnp.bfloat16
    dma = pltpu.SemaphoreType.DMA
    stride = 2 * kept
    mm, modes = pl.pallas_call(
        functools.partial(fused_kernel, n, local, chans, uniq, kept, rank),
        out_shape=(
            pltpu.VMEM((tiles, local * width, LANES), f32),
            pltpu.VMEM((2, kept, local), f32),
        ),
        in_specs=[hbm] * 4 + [vmem] * 2,
        out_specs=(pl.BlockSpec(memory_space=pltpu.VMEM), vmem),
        scratch_shapes=[
            pltpu.VMEM((steps, slab, RADIX, 2, per, LANES), f32),
            pltpu.VMEM((steps + 2, slab, RADIX, 2, per, LANES), f32),
            pltpu.VMEM((RADIX, total, LANES), f32),
            pltpu.VMEM((steps, RADIX, total, LANES), f32),
            pltpu.VMEM((steps, RADIX, total, LANES), f32),
            pltpu.VMEM((RADIX, dec.shape[2], LANES), f32),
            pltpu.VMEM((local * stride, LANES), f32),
            pltpu.VMEM((2, kept * chans, LANES), f32),
            pltpu.VMEM(enc.shape, bf16),
            pltpu.VMEM(dec.shape, bf16),
            dma((BLOCKS,)),
            dma((2,)),
            dma((steps,)),
            dma((steps,)),
            dma,
            dma((steps,)),
            dma,
            dma((steps + 1,)),
            dma((tiles,)),
        ],
        compiler_params=pltpu.CompilerParams(
            collective_id=0, has_side_effects=True, vmem_limit_bytes=62_700_000
        ),
        name="fused",
    )(
        visibilities.reshape(local // RADIX, RADIX, width, raw),
        filters, enc, dec, redundancy.reshape(1, raw), mode_counts.reshape(1, local),
    )
    chunks = 8
    mmodes, modes = pl.pallas_call(
        emit_kernel,
        out_shape=(
            jax.ShapeDtypeStruct((local * width, uniq), f32),
            jax.ShapeDtypeStruct((2, kept, local), f32),
        ),
        in_specs=[vmem, vmem],
        out_specs=(hbm, vmem),
        scratch_shapes=[dma((tiles, chunks))],
        compiler_params=pltpu.CompilerParams(vmem_limit_bytes=32 * 2**20),
        name="emit",
    )(mm, modes)
    return mmodes.reshape(local, 2, chans, uniq), jnp.transpose(modes, (2, 0, 1))


def phase_table(numer, period):
    phases = 2.0 * jnp.pi / period * numer.astype(jnp.float32)
    return (jnp.cos(phases), jnp.sin(phases))


def apply_stacked(cosine, sine_table, stacked, width):
    cos_part = jnp.dot(
        cosine, stacked, precision=lax.Precision.HIGHEST, preferred_element_type=jnp.float32
    )
    sin_part = jnp.dot(
        sine_table, stacked, precision=lax.Precision.HIGHEST, preferred_element_type=jnp.float32
    )
    real_out = cos_part[:, :width] + sin_part[:, width:]
    imag_out = cos_part[:, width:] - sin_part[:, :width]
    return jnp.concatenate([real_out, imag_out], axis=1)


def factored_transform(stacked, width):
    length = stacked.shape[0]
    radix_size = 64
    inner_size = length // radix_size
    outer_row = lax.broadcasted_iota(jnp.int32, (radix_size, radix_size), 0)
    outer_col = lax.broadcasted_iota(jnp.int32, (radix_size, radix_size), 1)
    cosine, sine_table = phase_table(outer_row * outer_col % radix_size, radix_size)
    grouped = stacked.reshape(radix_size, inner_size, 2, width)
    grouped = jnp.transpose(grouped, (0, 2, 1, 3)).reshape(radix_size, 2 * inner_size * width)
    section = apply_stacked(cosine, sine_table, grouped, inner_size * width)
    section = section.reshape(radix_size, 2, inner_size, width)
    section_real = section[:, 0]
    section_imag = section[:, 1]
    twist_row = lax.broadcasted_iota(jnp.int32, (radix_size, inner_size, 1), 0)
    twist_col = lax.broadcasted_iota(jnp.int32, (radix_size, inner_size, 1), 1)
    twist_cos, twist_sin = phase_table(twist_row * twist_col, length)
    turned_real = section_real * twist_cos + section_imag * twist_sin
    turned_imag = section_imag * twist_cos - section_real * twist_sin
    turned = jnp.stack([turned_real, turned_imag], axis=0)
    turned = jnp.transpose(turned, (2, 0, 1, 3)).reshape(inner_size, 2 * radix_size * width)
    inner_row = lax.broadcasted_iota(jnp.int32, (inner_size, inner_size), 0)
    inner_col = lax.broadcasted_iota(jnp.int32, (inner_size, inner_size), 1)
    cosine2, sine_table2 = phase_table(inner_row * inner_col % inner_size, inner_size)
    final = apply_stacked(cosine2, sine_table2, turned, radix_size * width)
    final = final.reshape(inner_size, 2, radix_size, width)
    return jnp.transpose(final, (0, 2, 1, 3)).reshape(length, 2 * width)


def transform(columns):
    length, _, width = columns.shape
    stacked = columns.reshape(length, 2 * width)
    result = factored_transform(stacked, width)
    scale = 1.0 / jnp.sqrt(jnp.float32(length))
    return (result * scale).reshape(length, 2, width)


def on_device(visibilities, redundancy, mode_counts, filters):
    groups = lax.axis_size("tm")
    local_times, _, channels, raw_count = visibilities.shape
    uniques = filters.shape[4]
    kept = filters.shape[2]
    if fits(groups, local_times, channels, raw_count, uniques, kept):
        return fused_device(visibilities, redundancy, mode_counts, filters)
    unique_block = uniques // groups
    members = (
        redundancy[:, None] == lax.broadcasted_iota(jnp.int32, (raw_count, uniques), 1)
    ).astype(jnp.float32)
    weights = members / jnp.sum(members, axis=0, keepdims=True)
    flat_rows = visibilities.reshape(local_times, 2 * channels, raw_count)
    blocked_weights = weights.reshape(raw_count, groups, unique_block)
    packed = jnp.einsum(
        "tqr,rjc->tjqc",
        flat_rows,
        blocked_weights,
        precision=lax.Precision.HIGHEST,
        preferred_element_type=jnp.float32,
    )
    packed = packed.reshape(local_times, groups, 2 * channels * unique_block)
    arrived = lax.all_to_all(packed, "tm", split_axis=1, concat_axis=0, tiled=True)
    length = arrived.shape[0]
    spectra = transform(arrived.reshape(length, 2, channels * unique_block))
    spectra = spectra.reshape(length, 1, 2 * channels * unique_block)
    regrouped = lax.all_to_all(spectra, "tm", split_axis=0, concat_axis=1, tiled=True)
    regrouped = regrouped.reshape(local_times, groups, 2, channels, unique_block)
    mmodes = jnp.transpose(regrouped, (0, 2, 3, 1, 4)).reshape(local_times, 2, channels, uniques)
    local_modes = mmodes.shape[0]
    rounded = mmodes.astype(jnp.bfloat16).reshape(local_modes, 2, channels * uniques)
    flat_filters = filters.reshape(local_modes, 2, kept, channels * uniques)
    products = jnp.einsum(
        "mpkc,mqc->mpqk", flat_filters, rounded, preferred_element_type=jnp.float32
    )
    real_out = products[:, 0, 0] - products[:, 1, 1]
    imag_out = products[:, 0, 1] + products[:, 1, 0]
    kept_mask = lax.broadcasted_iota(jnp.int32, (local_modes, kept), 1) < mode_counts[:, None]
    modes = jnp.where(kept_mask[:, None, :], jnp.stack([real_out, imag_out], axis=1), 0.0)
    return (mmodes, modes)


def solution(mesh):
    return jax.shard_map(
        on_device,
        mesh=mesh,
        in_specs=(P("tm", None, "grp", None), P("grp"), P("tm"), P("tm", None, None, "grp", None)),
        out_specs=(P("tm", None, "grp", None), P("tm", None, "grp")),
        check_vma=False,
    )
```
